128 devices in a mesh: slab: 16 (over z, y), blk: 8 (over x, core).
Axes of the slice: x: 4, y: 4, z: 4, core: 2. Of those that a mesh axis runs over, the one named last changes fastest.
Arguments:
- positions: float32 [4096, 3, 128], P(('slab', 'blk')), may hold values from 0 to 1
- radius: float32 [4096, 128], P(('slab', 'blk')), may hold values from 0.15 to 0.3
- velocity: float32 [4096, 3, 128], P(('slab', 'blk')), may hold values from -3 to 3
- old_force: float32 [4096, 3, 128], P(('slab', 'blk')), may hold values from -6 to 6
- neighbours: int32 [4096, 16], P(('slab', 'blk')), may hold values from 0 to 47, as said below
- tile_count: int32 [4096], P(('slab', 'blk')), may hold values from 0 to 16
Outputs:
- new_positions: float32 [4096, 3, 128], P(('slab', 'blk'))
- new_velocity: float32 [4096, 3, 128], P(('slab', 'blk'))
- new_force: float32 [4096, 3, 128], P(('slab', 'blk'))
The draws below stay inside these ranges and needn't reach their ends.
Inputs may be any that keep to these rules, and one draw needn't show every extreme that they name: neighbours[i, k] indexes the candidate list of bin i's group; it never names bin i itself, and names no candidate of a missing slab at the drum's ends.
All inputs are finite; a program needn't handle non-finite values.
Results may differ from the reference program's by a relative error of at most 0.0003.
Values sent between devices are 32-bit elements; how exact they have to be, the bound alone decides.
No kernel may reach another device: no remote copies, remote signals or barrier semaphores. Data moves between devices by JAX's collectives and lax.ppermute only.
A program may use at most 64 MiB of HBM per device.

```python
import math
import jax
import jax.numpy as jnp
from jax import lax

SPHERES = 128
SLOTS = 16
GHOSTS = 8
BLOCK_TILES = 32
BINS_DEV = 32
NBINS = 4096
N_SLAB = 16
N_BLK = 8


def draw_tile_count(key, part):
    total_bins = N_SLAB * N_BLK * BINS_DEV
    row_index = jnp.arange(total_bins, dtype=jnp.int32)
    group_index = row_index // BINS_DEV
    slab_index = group_index // N_BLK
    sector = group_index % N_BLK
    offsets = jax.random.randint(jax.random.fold_in(key, 7), (N_SLAB,), 0, N_BLK)
    dense = (sector - offsets[slab_index]) % N_BLK < max(N_BLK // 4, 1)
    ceiling = jnp.where(dense, SLOTS, SLOTS // 4).astype(jnp.int32)
    counts = jax.random.randint(jax.random.fold_in(key, 11), (total_bins,), 0, ceiling + 1)
    first_bin = row_index % BINS_DEV == 0
    counts = jnp.where(first_bin, jnp.where(dense, SLOTS, 0), counts)
    return counts.astype(jnp.int32)


def draw_neighbours(key, part):
    total_bins = N_SLAB * N_BLK * BINS_DEV
    row_index = jnp.arange(total_bins, dtype=jnp.int32)
    slab_index = row_index // BINS_DEV // N_BLK
    local_bin = row_index % BINS_DEV
    lowest = jnp.where(slab_index == 0, GHOSTS, 0).astype(jnp.int32)
    highest = jnp.where(slab_index == N_SLAB - 1, GHOSTS + BINS_DEV, BINS_DEV + 2 * GHOSTS).astype(jnp.int32)
    drawn = jax.random.randint(jax.random.fold_in(key, 13), (total_bins, SLOTS), 0, (highest - lowest - 1)[:, None])
    chosen = lowest[:, None] + drawn
    itself = (GHOSTS + local_bin)[:, None]
    chosen = jnp.where(chosen >= itself, chosen + 1, chosen)
    return chosen.astype(jnp.int32)


def block_scale(stream_key, dims, pieces, smallest, largest):
    def one(position, shards_of):
        steps = jax.random.uniform(jax.random.fold_in(jax.random.fold_in(stream_key, 6), position), (shards_of,), jnp.float32, smallest / len(pieces), largest / len(pieces))
        return jnp.repeat(jnp.exp(steps), dims[position] // shards_of).reshape((-1,) + (1,) * (len(dims) - position - 1))

    level = one(*pieces[0])
    for cut in pieces[1:]:
        level = level * one(*cut)
    return level


def normal_values(own_key, extent, scale, bound, pieces=(), held_as=jnp.bfloat16):
    level = block_scale(own_key, extent, pieces, -0.22, 0.18) if pieces else 1.0
    entries = jax.random.normal(own_key, extent, jnp.float32) * scale * level
    return jnp.minimum(jnp.maximum(entries, -bound), bound).astype(held_as)


def setup_inputs(seed: int = 0) -> dict:
    seeds = jax.random.split(jax.random.key(seed), 7)
    positions = jnp.clip(1.0 * jax.random.uniform(seeds[0], (NBINS, 3, SPHERES), jnp.float32) ** block_scale(seeds[0], (NBINS, 3, SPHERES), ((0, 128),), -0.2, 0.2), 0.0, 1.0)
    radius = jnp.clip(jnp.exp(math.log(0.3) - 0.6931472 * jax.random.uniform(seeds[1], (NBINS, SPHERES), jnp.float32) ** block_scale(seeds[1], (NBINS, SPHERES), ((0, 128),), -0.2, 0.2)), 0.15, 0.3)
    velocity = normal_values(seeds[2], (NBINS, 3, SPHERES), 0.5, 3.0, ((0, 128),), jnp.float32)
    old_force = normal_values(seeds[3], (NBINS, 3, SPHERES), 1.0, 6.0, ((0, 128),), jnp.float32)
    neighbours = draw_neighbours(jax.random.fold_in(seeds[6], 71), 0)
    tile_count = draw_tile_count(jax.random.fold_in(seeds[6], 71), 0)
    return {"positions": positions, "radius": radius, "velocity": velocity, "old_force": old_force, "neighbours": neighbours, "tile_count": tile_count}


STIFFNESS = 10.0
SOFTENING = 0.0025
TIMESTEP = 0.2

def pair_forces(left_tiles, right_tiles):
    offset_vec = left_tiles[:, :3, :, None] - right_tiles[:, :3, None, :]
    distance = jnp.sqrt(lax.optimization_barrier(jnp.sum(offset_vec * offset_vec, axis=1)) + SOFTENING)
    rad_left = left_tiles[:, 3, :, None]
    rad_right = right_tiles[:, 3, None, :]
    intersection = jnp.maximum(rad_left + rad_right - distance, 0.0)
    reduced = rad_left * rad_right / (rad_left + rad_right)
    magnitude = STIFFNESS * jnp.sqrt(reduced * intersection) * intersection / distance
    weighted = magnitude[:, None, :, :] * offset_vec
    return (lax.optimization_barrier(jnp.sum(weighted, axis=3)), -lax.optimization_barrier(jnp.sum(weighted, axis=2)))

def acceleration(force, radius):
    body_mass = 125.0 * radius * radius * radius
    gravity_term = jnp.zeros_like(force).at[:, 1, :].set(-0.5)
    return force / body_mass[:, None, :] + gravity_term

def device_forces(extended, neighbour_rows, live_count):
    own_bins = extended[GHOSTS:GHOSTS + BINS_DEV]
    self_force = lax.map(lambda inputs: pair_forces(inputs, inputs)[0], own_bins.reshape(BINS_DEV // BLOCK_TILES, BLOCK_TILES, 4, SPHERES))
    self_force = self_force.reshape(BINS_DEV, 3, SPHERES)
    flat_index = neighbour_rows.reshape(-1).astype(jnp.int32)
    left_tiles = jnp.repeat(own_bins, SLOTS, axis=0)
    right_tiles = jnp.take(extended, flat_index, axis=0)
    live_mask = (jnp.arange(SLOTS, dtype=jnp.int32)[None, :] < live_count[:, None]).reshape(-1).astype(extended.dtype)
    tile_blocks = BINS_DEV * SLOTS // BLOCK_TILES

    def block_forces(inputs):
        force_left, force_right = pair_forces(inputs[0], inputs[1])
        return (force_left * inputs[2][:, None, None], force_right * inputs[2][:, None, None])
    force_left, force_right = lax.map(block_forces, (left_tiles.reshape(tile_blocks, BLOCK_TILES, 4, SPHERES), right_tiles.reshape(tile_blocks, BLOCK_TILES, 4, SPHERES), live_mask.reshape(tile_blocks, BLOCK_TILES)))
    force_left = force_left.reshape(BINS_DEV, SLOTS, 3, SPHERES)
    force_right = force_right.reshape(BINS_DEV * SLOTS, 3 * SPHERES)
    candidate = BINS_DEV + 2 * GHOSTS
    onehot = (flat_index[:, None] == jnp.arange(candidate, dtype=jnp.int32)[None, :]).astype(extended.dtype)
    reaction = jnp.einsum('me,mf->ef', onehot, force_right, precision=lax.Precision.HIGHEST)
    reaction = reaction.reshape(candidate, 3, SPHERES)
    own_force = self_force + lax.optimization_barrier(jnp.sum(force_left, axis=1)) + reaction[GHOSTS:GHOSTS + BINS_DEV]
    return (own_force, reaction[:GHOSTS], reaction[GHOSTS + BINS_DEV:])

def reference(positions, radius, velocity, old_force, neighbours, tile_count):
    groups = N_SLAB * N_BLK
    accel_old = acceleration(old_force, radius)
    new_positions = positions + TIMESTEP * velocity + 0.5 * TIMESTEP * TIMESTEP * accel_old
    packed = jnp.concatenate([new_positions, radius[:, None, :]], axis=1)
    bin_grid = packed.reshape(N_SLAB, N_BLK, BINS_DEV, 4, SPHERES)
    empty_slab = jnp.zeros_like(bin_grid[:1])
    from_below = jnp.concatenate([empty_slab, bin_grid[:-1]], axis=0)[:, :, BINS_DEV - GHOSTS:]
    from_above = jnp.concatenate([bin_grid[1:], empty_slab], axis=0)[:, :, :GHOSTS]
    extended = jnp.concatenate([from_below, bin_grid, from_above], axis=2)
    extended = extended.reshape(groups, BINS_DEV + 2 * GHOSTS, 4, SPHERES)
    own_force, lower_part, upper_part = lax.map(lambda inputs: device_forces(inputs[0], inputs[1], inputs[2]), (extended, neighbours.reshape(groups, BINS_DEV, SLOTS), tile_count.reshape(groups, BINS_DEV)))
    own_force = own_force.reshape(N_SLAB, N_BLK, BINS_DEV, 3, SPHERES)
    lower_part = lower_part.reshape(N_SLAB, N_BLK, GHOSTS, 3, SPHERES)
    upper_part = upper_part.reshape(N_SLAB, N_BLK, GHOSTS, 3, SPHERES)
    own_force = own_force.at[:-1, :, BINS_DEV - GHOSTS:].add(lower_part[1:])
    own_force = own_force.at[1:, :, :GHOSTS].add(upper_part[:-1])
    new_force = own_force.reshape(N_SLAB * N_BLK * BINS_DEV, 3, SPHERES)
    new_velocity = velocity + 0.5 * TIMESTEP * (accel_old + acceleration(new_force, radius))
    return (new_positions, new_velocity, new_force)
```

```python
import functools

import jax
import jax.numpy as jnp
from jax import lax
from jax.experimental import pallas as pl
from jax.experimental.pallas import tpu as pltpu
from jax.sharding import PartitionSpec as P

GHOSTS = 8
TIMESTEP = 0.2
TINY = 1e-25
TILES = 4
BINS = 32
OWN_END = BINS * BINS
SIDE = BINS * GHOSTS
CROSS_END = 4 * SIDE
F32 = jnp.float32
BF16 = jnp.bfloat16


def split3(value):
    high = value.astype(BF16).astype(F32)
    middle = (value - high).astype(BF16).astype(F32)
    return high, middle, value - high - middle


def write_rows(packed, base, left, right, moment):
    span = pl.ds(base, BINS)
    radius = packed[:BINS, 3, :]
    sigma = jnp.sqrt(10.0 * radius)
    one = jnp.ones((BINS, 128), F32)
    zero = jnp.zeros((BINS, 128), F32)
    norm = zero
    for c in range(3):
        place = packed[:BINS, c, :] - 0.5
        norm = norm + place * place
        h, m, l = split3(place)
        if left is not None:
            for t, value in enumerate((h, h, h, m, m, l)):
                left[:, 6 * c + t, :] = value
        for t, value in enumerate((h, m, l, h, m, h)):
            right[span, 6 * c + t, :] = -2.0 * value
        for t, value in enumerate(split3(sigma * place)):
            moment[span, 3 * c + t, :] = value
    for t, value in enumerate(split3(sigma)):
        moment[span, 9 + t, :] = value
    for t in range(12, 16):
        moment[span, t, :] = zero
    for t, value in enumerate(split3(norm + 0.0025)):
        right[span, 18 + t, :] = one
        right[span, 21 + t, :] = value
    for t in range(24, 32):
        right[span, t, :] = zero
    if left is not None:
        for t, value in enumerate(split3(norm)):
            left[:, 18 + t, :] = value
            left[:, 21 + t, :] = one
        for t, value in enumerate(split3(radius)):
            left[:, 24 + t, :] = value
        for t in range(27, 32):
            left[:, t, :] = zero


def narrow(count, rows, out):
    def step(n, carry):
        out[n] = rows[n].astype(BF16)
        return carry

    lax.fori_loop(0, count, step, 0, unroll=4)


def run_tiles(end, decode, weight, following, lt, ra, right, moment, radius, acc_a, acc_b, scratch):
    s0, s1, p0, p1 = scratch
    for ref in (s0, s1):
        ref[...] = jnp.ones_like(ref)
    for ref in (p0, p1):
        ref[...] = jnp.zeros_like(ref)

    def distances(tiles, s_ref):
        for n, f in enumerate(tiles):
            a, b = decode(f)[:2]
            s_ref[n] = jnp.dot(lt[a], right[b], preferred_element_type=F32)

    def weights(tiles, s_ref, p_ref):
        for n, f in enumerate(tiles):
            a, b = decode(f)[:2]
            scale = weight[f]
            r_b = radius(b)
            for g in range(8):
                rows = slice(16 * g, 16 * g + 16)
                s = s_ref[n, rows, :]
                t = (ra[a, rows, :] + r_b) * lax.rsqrt(s)
                v = jnp.maximum(t - 1.0, TINY)
                w = (v * scale) * v * lax.rsqrt(v * t)
                high = w.astype(BF16)
                low = (w - high.astype(F32)).astype(BF16)
                p_ref[n, rows, :128] = high
                p_ref[n, rows, 128:] = low

    def forces(tiles, p_ref):
        for q in range(0, TILES, 2):
            a1, b1, c1 = decode(tiles[q])
            a2, b2, c2 = decode(tiles[q + 1])
            first, second = p_ref[q], p_ref[q + 1]
            if acc_b is not None:
                m = jnp.concatenate([moment[a1], moment[a2]], axis=0)
                both = jnp.concatenate(
                    [
                        jnp.concatenate([first[:, :128], second[:, :128]], axis=1),
                        jnp.concatenate([first[:, 128:], second[:, 128:]], axis=1),
                    ],
                    axis=0,
                )
                out = jnp.dot(
                    jnp.concatenate([m, m], axis=1), both, preferred_element_type=F32
                )
                acc_b[c1] += out[:16, :128]
                acc_b[c2] += out[16:, 128:]
            m = jnp.concatenate([moment[b1], moment[b2]], axis=0)
            out = lax.dot_general(
                jnp.concatenate([m, m], axis=1),
                jnp.concatenate([first, second], axis=0),
                (((1,), (1,)), ((), ())),
                preferred_element_type=F32,
            )
            acc_a[a1] += out[:16, :128]
            acc_a[a2] += out[16:, 128:]

    def draw(f):
        tiles = []
        for _ in range(TILES):
            tiles.append(f)
            f = following[jnp.minimum(f + 1, end)]
        return f, tuple(tiles)

    none = (jnp.int32(end),) * TILES

    def body(_, carry):
        f, second, third = carry
        f, first = draw(f)
        forces(third, p0)
        weights(second, s0, p1)
        distances(first, s1)
        f, fresh = draw(f)
        forces(second, p1)
        weights(first, s1, p0)
        distances(fresh, s0)
        return f, fresh, first

    live = following[end + 1]
    halves = (live + TILES - 1) // TILES + 2
    lax.fori_loop(0, (halves + 1) // 2, body, (following[0], none, none))


def own_kernel(weight, following, packed, acc, lt, ra, left, right, moment, right_b, moment_b, acc_b, *scratch):
    write_rows(packed, 0, left, right, moment)
    narrow(BINS, right, right_b)
    narrow(BINS, moment, moment_b)
    row = lax.broadcasted_iota(jnp.int32, (32, 128), 0)
    choose = ((row >= 24) & (row < 27)).astype(BF16)

    def turn(n, carry):
        columns = jnp.transpose(left[n]).astype(BF16)
        lt[n] = columns
        ra[n] = jnp.dot(columns, choose, preferred_element_type=F32)
        return carry

    lax.fori_loop(0, BINS, turn, 0, unroll=4)
    acc[...] = jnp.zeros_like(acc)
    acc_b[...] = jnp.zeros_like(acc_b)

    def decode(f):
        a = jnp.minimum(f >> 5, BINS - 1)
        b = f & (BINS - 1)
        return a, b, jnp.where(a == b, BINS, b)

    run_tiles(OWN_END, decode, weight, following, lt, ra, right_b, moment_b,
              lambda b: packed[b, pl.ds(3, 1), :], acc, acc_b, scratch)
    acc[...] += acc_b[:BINS]


def cross_kernel(weight, following, code, even, odd, packed, velocity, old_force, acc_in, lt, ra,
                 new_velocity, new_force, right, moment, right_b, moment_b, radii, acc, *scratch):
    write_rows(even, 0, None, right, moment)
    write_rows(odd, BINS, None, right, moment)
    radii[:BINS] = even[:BINS, pl.ds(3, 1), :]
    radii[BINS:] = odd[:BINS, pl.ds(3, 1), :]
    narrow(2 * BINS, right, right_b)
    narrow(2 * BINS, moment, moment_b)
    acc[...] = acc_in[...]

    def decode(f):
        c = code[f]
        return c >> 6, c & 63, 0

    run_tiles(CROSS_END, decode, weight, following, lt, ra, right_b, moment_b,
              lambda b: radii[b], acc, None, scratch)
    radius = packed[:BINS, 3, :]
    sigma = jnp.sqrt(10.0 * radius)
    mass = 125.0 * radius * radius * radius
    total = acc[:, 9, :] + acc[:, 10, :] + acc[:, 11, :]
    for c in range(3):
        moment_c = acc[:, 3 * c, :] + acc[:, 3 * c + 1, :] + acc[:, 3 * c + 2, :]
        force = sigma * ((packed[:BINS, c, :] - 0.5) * total - moment_c)
        new_force[:, c, :] = force
        gravity = -0.5 if c == 1 else 0.0
        accel = (old_force[:, c, :] / mass + gravity) + (force / mass + gravity)
        new_velocity[:, c, :] = velocity[:, c, :] + 0.5 * TIMESTEP * accel


VMEM = pl.BlockSpec(memory_space=pltpu.VMEM)
SMEM = pl.BlockSpec(memory_space=pltpu.SMEM)


def pipeline_scratch():
    return [
        pltpu.VMEM((TILES, 128, 128), F32),
        pltpu.VMEM((TILES, 128, 128), F32),
        pltpu.VMEM((TILES, 128, 256), BF16),
        pltpu.VMEM((TILES, 128, 256), BF16),
    ]


def acceleration(force, radius):
    body_mass = 125.0 * radius * radius * radius
    gravity_term = jnp.zeros_like(force).at[:, 1, :].set(-0.5)
    return force / body_mass[:, None, :] + gravity_term


def next_live(live):
    length = live.shape[-1]
    here = lax.broadcasted_iota(jnp.int32, (length, length), 0)
    there = lax.broadcasted_iota(jnp.int32, (length, length), 1)
    return jnp.min(
        jnp.where((there >= here) & live[..., None, :], there, length), axis=-1
    )


def local(positions, radius, velocity, old_force, neighbours, tile_count):
    new_positions = positions + TIMESTEP * velocity + 0.5 * TIMESTEP * TIMESTEP * acceleration(old_force, radius)
    slots = neighbours.shape[1]
    live = lax.broadcasted_iota(jnp.int32, (BINS, slots), 1) < tile_count[:, None]
    marked = jnp.where(live, neighbours, -1)
    candidates = BINS + 2 * GHOSTS
    counts = jnp.sum(
        (marked[:, :, None] == lax.broadcasted_iota(jnp.int32, (1, 1, candidates), 2)).astype(F32), axis=1
    )
    sides = jnp.stack([counts[:, :GHOSTS].reshape(-1), counts[:, GHOSTS + BINS :].reshape(-1)])
    side_next = next_live(sides > 0.0)
    lists = jnp.concatenate([sides, side_next.astype(F32)]).reshape(2, 4, 128)
    packed = jnp.concatenate([jnp.concatenate([new_positions, radius[:, None, :]], axis=1), lists])

    slabs = lax.axis_size("slab")
    swap_even = [(i + d, i + 1 - d) for i in range(0, slabs - 1, 2) for d in (0, 1)]
    swap_odd = [(i + d, i + 1 - d) for i in range(1, slabs - 1, 2) for d in (0, 1)]
    even = lax.ppermute(packed, "slab", swap_even)
    odd = lax.ppermute(packed, "slab", swap_odd)

    inner = counts[:, GHOSTS : GHOSTS + BINS]
    row = lax.broadcasted_iota(jnp.int32, (BINS, BINS), 0)
    column = lax.broadcasted_iota(jnp.int32, (BINS, BINS), 1)
    own = jnp.where(column > row, inner + inner.T, jnp.where(column == row, 1.0, 0.0))
    place = row * BINS + column
    first = jnp.min(jnp.where(own > 0.0, place, OWN_END), axis=1)
    later = jnp.min(jnp.where(column > row, first[None, :], OWN_END), axis=1)
    within = jnp.min(
        jnp.where(
            (column[None] >= row[None]) & (own > 0.0)[:, None, :], place[:, None, :], OWN_END
        ),
        axis=2,
    )
    own_next = jnp.minimum(within, later[:, None]).reshape(-1)
    own_live = jnp.sum((own > 0.0).astype(jnp.int32))
    end = jnp.full((1,), OWN_END, jnp.int32)
    own_next = jnp.concatenate([own_next, end, own_live[None], jnp.zeros((126,), jnp.int32)])
    own_weight = jnp.concatenate([own.reshape(-1), jnp.zeros((128,), F32)])

    acc, lt, ra = pl.pallas_call(
        own_kernel,
        out_shape=(
            jax.ShapeDtypeStruct((BINS, 16, 128), F32),
            jax.ShapeDtypeStruct((BINS, 128, 32), BF16),
            jax.ShapeDtypeStruct((BINS, 128, 128), F32),
        ),
        in_specs=[SMEM, SMEM, VMEM],
        out_specs=(VMEM, VMEM, VMEM),
        scratch_shapes=[
            pltpu.VMEM((BINS, 32, 128), F32),
            pltpu.VMEM((BINS, 32, 128), F32),
            pltpu.VMEM((BINS, 16, 128), F32),
            pltpu.VMEM((BINS, 32, 128), BF16),
            pltpu.VMEM((BINS, 16, 128), BF16),
            pltpu.VMEM((BINS + 1, 16, 128), F32),
            *pipeline_scratch(),
        ],
        compiler_params=pltpu.CompilerParams(vmem_limit_bytes=16 << 20),
        cost_estimate=pl.CostEstimate(flops=10**9, bytes_accessed=10**6, transcendentals=0),
        name="own_tiles",
    )(own_weight, own_next, packed)

    lists_even = even[BINS:].reshape(2, 2, SIDE)
    lists_odd = odd[BINS:].reshape(2, 2, SIDE)
    above_even = lax.axis_index("slab") % 2 == 0
    from_below = jnp.where(above_even, lists_odd[:, 1], lists_even[:, 1])
    from_above = jnp.where(above_even, lists_even[:, 0], lists_odd[:, 0])
    cross_weight = jnp.concatenate([sides, from_below[None, 0], from_above[None, 0]])
    steps = jnp.concatenate(
        [side_next, from_below[None, 1].astype(jnp.int32), from_above[None, 1].astype(jnp.int32)]
    )
    start = jnp.int32(CROSS_END)
    chained = []
    for n in (3, 2, 1, 0):
        row_steps = jnp.where(steps[n] < SIDE, steps[n] + n * SIDE, start)
        row_steps = jnp.where(jnp.max(cross_weight[n]) > 0.0, row_steps, start)
        start = row_steps[0]
        chained.insert(0, row_steps)
    cross_live = jnp.sum((cross_weight > 0.0).astype(jnp.int32))
    end = jnp.full((1,), CROSS_END, jnp.int32)
    cross_next = jnp.concatenate(chained + [end, cross_live[None], jnp.zeros((126,), jnp.int32)])
    cross_weight = jnp.concatenate([cross_weight.reshape(-1), jnp.zeros((128,), F32)])
    index = lax.broadcasted_iota(jnp.int32, (BINS, GHOSTS), 0)
    ghost = lax.broadcasted_iota(jnp.int32, (BINS, GHOSTS), 1)
    below = jnp.where(above_even, BINS, 0)
    above = BINS - below
    code = jnp.concatenate(
        [
            (index * 64 + below + BINS - GHOSTS + ghost).reshape(-1),
            (index * 64 + above + ghost).reshape(-1),
            (ghost * 64 + below + index).reshape(-1),
            ((BINS - GHOSTS + ghost) * 64 + above + index).reshape(-1),
            jnp.zeros((128,), jnp.int32),
        ]
    )
    new_velocity, new_force = pl.pallas_call(
        cross_kernel,
        out_shape=(
            jax.ShapeDtypeStruct((BINS, 3, 128), F32),
            jax.ShapeDtypeStruct((BINS, 3, 128), F32),
        ),
        in_specs=[SMEM, SMEM, SMEM] + [VMEM] * 8,
        out_specs=(VMEM, VMEM),
        scratch_shapes=[
            pltpu.VMEM((2 * BINS, 32, 128), F32),
            pltpu.VMEM((2 * BINS, 16, 128), F32),
            pltpu.VMEM((2 * BINS, 32, 128), BF16),
            pltpu.VMEM((2 * BINS, 16, 128), BF16),
            pltpu.VMEM((2 * BINS, 1, 128), F32),
            pltpu.VMEM((BINS, 16, 128), F32),
            *pipeline_scratch(),
        ],
        compiler_params=pltpu.CompilerParams(vmem_limit_bytes=16 << 20),
        cost_estimate=pl.CostEstimate(flops=10**9, bytes_accessed=10**6, transcendentals=0),
        name="cross_tiles",
    )(cross_weight, cross_next, code, even, odd, packed, velocity, old_force, acc, lt, ra)
    return (new_positions, new_velocity, new_force)


def solution(mesh):
    flat = P(("slab", "blk"))
    rows = P(("slab", "blk"), None)
    cells = P(("slab", "blk"), None, None)
    return jax.shard_map(
        local,
        mesh=mesh,
        in_specs=(cells, rows, cells, cells, rows, flat),
        out_specs=(cells, cells, cells),
        check_vma=False,
    )
```

```python
import jax
import jax.numpy as jnp
from jax import lax
from jax.experimental import pallas as pl
from jax.experimental.pallas import tpu as pltpu
from jax.sharding import PartitionSpec as P

GHOSTS = 8
TIMESTEP = 0.2
TINY = 1e-25
TILES = 4
BINS = 32
DEPTH = 48
END = BINS * 128
PLACES = 8192
F32 = jnp.float32
BF16 = jnp.bfloat16


def rounded(value):
    return value.astype(BF16).astype(F32)


def split3(value):
    high = rounded(value)
    middle = rounded(value - high)
    return high, middle, value - high - middle


def iotas(rows):
    shape = (rows, 128)
    return lax.broadcasted_iota(jnp.int32, shape, 0), lax.broadcasted_iota(jnp.int32, shape, 1)


def widened(value):
    rows, lanes = value.shape
    return jnp.concatenate([value, jnp.zeros((rows, 128 - lanes), value.dtype)], axis=1)


def table_of(weight):
    row, lane = iotas(BINS)
    step = jnp.where(weight > 0.0, row * 128 + lane, END)
    for s in (1, 2, 4, 8, 16, 32, 64):
        ahead = pltpu.roll(step, 128 - s, 1)
        step = jnp.minimum(step, jnp.where(lane + s < 128, ahead, END))
    later = jnp.broadcast_to(step[:, :1], (BINS, 128))
    later = jnp.where(row + 1 < BINS, pltpu.roll(later, BINS - 1, 0), END)
    for s in (1, 2, 4, 8, 16):
        ahead = pltpu.roll(later, BINS - s, 0)
        later = jnp.minimum(later, jnp.where(row + s < BINS, ahead, END))
    live = jnp.sum(jnp.where(weight > 0.0, 1.0, 0.0), axis=1, keepdims=True)
    live = jnp.broadcast_to(jnp.sum(live, axis=0, keepdims=True), (8, 128)).astype(jnp.int32)
    tail, _ = iotas(8)
    tail = jnp.where(tail == 1, live, END)
    return jnp.concatenate([jnp.minimum(step, later) + PLACES * weight.astype(jnp.int32), tail])


def prologue_kernel(positions, velocity, old_force, radius, neighbours, count, new_positions, packed, table):
    r = radius[...]
    mass = 125.0 * r * r * r
    for c in range(3):
        accel = old_force[c] / mass + (-0.5 if c == 1 else 0.0)
        place = positions[c] + TIMESTEP * velocity[c] + 0.5 * TIMESTEP * TIMESTEP * accel
        new_positions[c] = place
        packed[:BINS, c, :] = place
    packed[:BINS, 3, :] = r
    slots = neighbours.shape[0]
    slot = lax.broadcasted_iota(jnp.int32, (slots, BINS), 0)
    marked = jnp.where(slot < count[...], neighbours[...], -1).astype(F32)
    marked = jnp.transpose(widened(marked))[:BINS]
    row, lane = iotas(BINS)
    candidate = lane.astype(F32)
    counts = jnp.zeros((BINS, 128), F32)
    for k in range(slots):
        counts = counts + jnp.where(marked[:, k : k + 1] == candidate, 1.0, 0.0)
    for n in range(BINS // 4):
        packed[BINS + n] = counts[4 * n : 4 * n + 4]
    inner = jnp.where(lane < BINS, pltpu.roll(counts, 128 - GHOSTS, 1), 0.0)
    mirror = widened(jnp.transpose(inner)[:BINS])
    pairs = jnp.where(lane > row, inner + mirror, 0.0)
    table[...] = table_of(jnp.where(lane == row, 1.0, pairs))


def write_rows(packed, base, left, right, moment):
    span = pl.ds(base, BINS)
    radius = packed[:BINS, 3, :]
    sigma = jnp.sqrt(10.0 * radius)
    one = jnp.ones((BINS, 128), F32)
    zero = jnp.zeros((BINS, 128), F32)
    norm = zero
    for c in range(3):
        place = packed[:BINS, c, :] - 0.5
        norm = norm + place * place
        right[span, c, :] = -2.0 * place
        moment[span, c, :] = sigma * place
        if left is not None:
            left[span, c, :] = place
    moment[span, 3, :] = sigma
    right[span, 3, :] = one
    right[span, 4, :] = norm + 0.0025
    for t in (5, 6, 7):
        right[span, t, :] = zero
    for t in (4, 5, 6, 7):
        moment[span, t, :] = zero
    if left is not None:
        left[span, 3, :] = norm
        left[span, 4, :] = one
        left[span, 5, :] = radius
        left[span, 6, :] = zero
        left[span, 7, :] = zero


def right_operands(n, right, moment, right_b, moment_b):
    high, middle, low = split3(right[n])
    right_b[n] = jnp.concatenate([high, middle, high, middle, low, high]).astype(BF16)
    high, middle, low = split3(moment[n])
    moment_b[n] = jnp.concatenate([high + pltpu.roll(middle, 4, 0), low]).astype(BF16)


def left_operand(n, left):
    high, middle, low = split3(left[n])
    return jnp.transpose(jnp.concatenate([high, high, middle, middle, high, low])).astype(BF16)


def run_tiles(table, target, lt, ra, right, moment, packed_row, acc_a, acc_b, scratch):
    s0, s1, p0, p1 = scratch
    for ref in (s0, s1):
        ref[...] = jnp.ones_like(ref)
    for ref in (p0, p1):
        ref[...] = jnp.zeros_like(ref)

    def bins(f):
        return jnp.minimum(f >> 7, BINS - 1), f & 127

    def distances(tiles, s_ref):
        for n, f in enumerate(tiles):
            a, b = bins(f)
            s_ref[n] = jnp.dot(lt[a], right[b], preferred_element_type=F32)

    def weights(tiles, s_ref, p_ref):
        for n, f in enumerate(tiles):
            a, b = bins(f)
            scale = (table[f >> 7, f & 127] >> 13).astype(F32)
            r_b = packed_row(b)
            for g in range(8):
                rows = slice(16 * g, 16 * g + 16)
                s = s_ref[n, rows, :]
                t = (ra[a, rows, :] + r_b) * lax.rsqrt(s)
                v = jnp.maximum(t - 1.0, TINY)
                w = (v * scale) * v * lax.rsqrt(v * t)
                high = w.astype(BF16)
                low = (w - high.astype(F32)).astype(BF16)
                p_ref[n, rows, :128] = high
                p_ref[n, rows, 128:] = low

    def forces(tiles, p_ref):
        for q in range(0, TILES, 2):
            a1, b1 = bins(tiles[q])
            a2, b2 = bins(tiles[q + 1])
            first, second = p_ref[q], p_ref[q + 1]
            if acc_b is not None:
                c1, c2 = target(a1, b1), target(a2, b2)
                m = jnp.concatenate([moment[a1], moment[a2]], axis=0)
                both = jnp.concatenate(
                    [
                        jnp.concatenate([first[:, :128], second[:, :128]], axis=1),
                        jnp.concatenate([first[:, 128:], second[:, 128:]], axis=1),
                    ],
                    axis=0,
                )
                out = jnp.dot(
                    jnp.concatenate([m, m], axis=1), both, preferred_element_type=F32
                )
                acc_b[c1] += out[:16, :128]
                acc_b[c2] += out[16:, 128:]
            m = jnp.concatenate([moment[b1], moment[b2]], axis=0)
            out = lax.dot_general(
                jnp.concatenate([m, m], axis=1),
                jnp.concatenate([first, second], axis=0),
                (((1,), (1,)), ((), ())),
                preferred_element_type=F32,
            )
            acc_a[a1] += out[:16, :128]
            acc_a[a2] += out[16:, 128:]

    def following(f):
        return table[f >> 7, f & 127] & (PLACES - 1)

    def draw(f):
        tiles = []
        for _ in range(TILES):
            tiles.append(f)
            f = following(jnp.minimum(f + 1, END))
        return f, tuple(tiles)

    none = (jnp.int32(END),) * TILES

    def body(_, carry):
        f, second, third = carry
        f, first = draw(f)
        forces(third, p0)
        weights(second, s0, p1)
        distances(first, s1)
        f, fresh = draw(f)
        forces(second, p1)
        weights(first, s1, p0)
        distances(fresh, s0)
        return f, fresh, first

    live = table[BINS + 1, 0]
    halves = (live + TILES - 1) // TILES + 2
    lax.fori_loop(0, (halves + 1) // 2, body, (following(jnp.int32(0)), none, none))


def own_kernel(table, packed, acc, lt, ra, left, right, moment, right_b, moment_b, acc_b, *scratch):
    write_rows(packed, 0, left, right, moment)
    depth = lax.broadcasted_iota(jnp.int32, (DEPTH, 128), 0)
    choose = ((depth == 5) | (depth == 21) | (depth == 45)).astype(BF16)

    def turn(n, carry):
        right_operands(n, right, moment, right_b, moment_b)
        columns = left_operand(n, left)
        lt[n] = columns
        ra[n] = jnp.dot(columns, choose, preferred_element_type=F32)
        return carry

    lax.fori_loop(0, BINS, turn, 0, unroll=8)
    acc[...] = jnp.zeros_like(acc)
    acc_b[...] = jnp.zeros_like(acc_b)
    run_tiles(table, lambda a, b: jnp.where(a == b, BINS, b), lt, ra, right_b, moment_b,
              lambda b: packed[b, pl.ds(3, 1), :], acc, acc_b, scratch)
    acc[...] += acc_b[:BINS]


def cross_kernel(upward, even, odd, packed, velocity, old_force, acc_in, lt, ra,
                 new_velocity, new_force, right, moment, right_b, moment_b, radii, acc,
                 table_v, table, *scratch):
    is_up = upward[0] > 0
    row, lane = iotas(BINS)

    def counts_of(ref):
        return jnp.concatenate([ref[BINS + n] for n in range(BINS // 4)])

    mine = counts_of(packed)
    lower = jnp.where((lane >= BINS - GHOSTS) & (lane < BINS), pltpu.roll(mine, BINS - GHOSTS, 1), 0.0)
    upper = jnp.where(lane < GHOSTS, pltpu.roll(mine, 128 - BINS - GHOSTS, 1), 0.0)
    blank = jnp.zeros((BINS - GHOSTS, 128), F32)

    def with_partner(counts, above):
        flipped = widened(jnp.transpose(counts))
        above_part = upper + jnp.concatenate([blank, flipped[:GHOSTS]])
        below_part = lower + jnp.concatenate([flipped[BINS + GHOSTS : BINS + 2 * GHOSTS], blank])
        return jnp.where(above, above_part, below_part)

    by_even = with_partner(counts_of(even), is_up)
    by_odd = with_partner(counts_of(odd), jnp.logical_not(is_up))
    table_v[...] = table_of(by_even + pltpu.roll(by_odd, BINS, 1))
    pltpu.sync_copy(table_v, table)
    write_rows(even, 0, None, right, moment)
    write_rows(odd, BINS, None, right, moment)
    radii[:BINS] = even[:BINS, pl.ds(3, 1), :]
    radii[BINS:] = odd[:BINS, pl.ds(3, 1), :]

    def turn(n, carry):
        right_operands(n, right, moment, right_b, moment_b)
        return carry

    lax.fori_loop(0, 2 * BINS, turn, 0, unroll=8)
    acc[...] = acc_in[...]
    run_tiles(table, None, lt, ra, right_b, moment_b, lambda b: radii[b], acc, None, scratch)
    radius = packed[:BINS, 3, :]
    sigma = jnp.sqrt(10.0 * radius)
    mass = 125.0 * radius * radius * radius

    def gathered(c):
        return acc[:, c, :] + acc[:, 4 + c, :] + acc[:, 8 + c, :]

    total = gathered(3)
    for c in range(3):
        force = sigma * ((packed[:BINS, c, :] - 0.5) * total - gathered(c))
        new_force[c] = force
        gravity = -0.5 if c == 1 else 0.0
        accel = (old_force[c] / mass + gravity) + (force / mass + gravity)
        new_velocity[c] = velocity[c] + 0.5 * TIMESTEP * accel


VMEM = pl.BlockSpec(memory_space=pltpu.VMEM)
SMEM = pl.BlockSpec(memory_space=pltpu.SMEM)


def pipeline_scratch():
    return [
        pltpu.VMEM((TILES, 128, 128), F32),
        pltpu.VMEM((TILES, 128, 128), F32),
        pltpu.VMEM((TILES, 128, 256), BF16),
        pltpu.VMEM((TILES, 128, 256), BF16),
    ]


def local(positions, radius, velocity, old_force, neighbours, tile_count):
    def by_component(cells):
        return jnp.transpose(cells, (1, 0, 2))

    positions, velocity, old_force = map(by_component, (positions, velocity, old_force))
    cells = jax.ShapeDtypeStruct((3, BINS, 128), F32)
    new_positions, packed, own_table = pl.pallas_call(
        prologue_kernel,
        out_shape=(
            cells,
            jax.ShapeDtypeStruct((BINS + 8, 4, 128), F32),
            jax.ShapeDtypeStruct((BINS + 8, 128), jnp.int32),
        ),
        in_specs=[VMEM] * 6,
        out_specs=(VMEM,) * 3,
        compiler_params=pltpu.CompilerParams(vmem_limit_bytes=8 << 20),
        name="prologue",
    )(positions, velocity, old_force, radius, neighbours.T, tile_count[None])

    slabs = lax.axis_size("slab")
    swap_even = [(i + d, i + 1 - d) for i in range(0, slabs - 1, 2) for d in (0, 1)]
    swap_odd = [(i + d, i + 1 - d) for i in range(1, slabs - 1, 2) for d in (0, 1)]
    even = lax.ppermute(packed, "slab", swap_even)
    odd = lax.ppermute(packed, "slab", swap_odd)

    acc, lt, ra = pl.pallas_call(
        own_kernel,
        out_shape=(
            jax.ShapeDtypeStruct((BINS, 16, 128), F32),
            jax.ShapeDtypeStruct((BINS, 128, DEPTH), BF16),
            jax.ShapeDtypeStruct((BINS, 128, 128), F32),
        ),
        in_specs=[SMEM, VMEM],
        out_specs=(VMEM, VMEM, VMEM),
        scratch_shapes=[
            pltpu.VMEM((BINS, 8, 128), F32),
            pltpu.VMEM((BINS, 8, 128), F32),
            pltpu.VMEM((BINS, 8, 128), F32),
            pltpu.VMEM((BINS, DEPTH, 128), BF16),
            pltpu.VMEM((BINS, 16, 128), BF16),
            pltpu.VMEM((BINS + 1, 16, 128), F32),
            *pipeline_scratch(),
        ],
        compiler_params=pltpu.CompilerParams(vmem_limit_bytes=16 << 20),
        cost_estimate=pl.CostEstimate(flops=10**9, bytes_accessed=10**6, transcendentals=0),
        name="own_tiles",
    )(own_table, packed)

    upward = (1 - lax.axis_index("slab") % 2).astype(jnp.int32)[None]
    new_velocity, new_force = pl.pallas_call(
        cross_kernel,
        out_shape=(cells, cells),
        in_specs=[SMEM] + [VMEM] * 8,
        out_specs=(VMEM, VMEM),
        scratch_shapes=[
            pltpu.VMEM((2 * BINS, 8, 128), F32),
            pltpu.VMEM((2 * BINS, 8, 128), F32),
            pltpu.VMEM((2 * BINS, DEPTH, 128), BF16),
            pltpu.VMEM((2 * BINS, 16, 128), BF16),
            pltpu.VMEM((2 * BINS, 1, 128), F32),
            pltpu.VMEM((BINS, 16, 128), F32),
            pltpu.VMEM((BINS + 8, 128), jnp.int32),
            pltpu.SMEM((BINS + 8, 128), jnp.int32),
            *pipeline_scratch(),
        ],
        compiler_params=pltpu.CompilerParams(vmem_limit_bytes=16 << 20),
        cost_estimate=pl.CostEstimate(flops=10**9, bytes_accessed=10**6, transcendentals=0),
        name="cross_tiles",
    )(upward, even, odd, packed, velocity, old_force, acc, lt, ra)
    return tuple(map(by_component, (new_positions, new_velocity, new_force)))


def solution(mesh):
    flat = P(("slab", "blk"))
    rows = P(("slab", "blk"), None)
    cells = P(("slab", "blk"), None, None)
    return jax.shard_map(
        local,
        mesh=mesh,
        in_specs=(cells, rows, cells, cells, rows, flat),
        out_specs=(cells, cells, cells),
        check_vma=False,
    )
```

```python
import jax
import jax.numpy as jnp
from jax import lax
from jax.experimental import pallas as pl
from jax.experimental.pallas import tpu as pltpu
from jax.sharding import PartitionSpec as P

GHOSTS = 8
TIMESTEP = 0.2
TINY = 1e-25
TILES = 4
BINS = 32
DEPTH = 48
END = BINS * 128
PLACES = 8192
HALVES = 4
F32 = jnp.float32
BF16 = jnp.bfloat16


def rounded(value):
    return value.astype(BF16).astype(F32)


def split3(value):
    high = rounded(value)
    middle = rounded(value - high)
    return high, middle, value - high - middle


def iotas(rows):
    shape = (rows, 128)
    return lax.broadcasted_iota(jnp.int32, shape, 0), lax.broadcasted_iota(jnp.int32, shape, 1)


def widened(value):
    rows, lanes = value.shape
    return jnp.concatenate([value, jnp.zeros((rows, 128 - lanes), value.dtype)], axis=1)


def table_of(weight):
    row, lane = iotas(BINS)
    step = jnp.where(weight > 0.0, row * 128 + lane, END)
    for s in (1, 2, 4, 8, 16, 32, 64):
        ahead = pltpu.roll(step, 128 - s, 1)
        step = jnp.minimum(step, jnp.where(lane + s < 128, ahead, END))
    later = jnp.broadcast_to(step[:, :1], (BINS, 128))
    later = jnp.where(row + 1 < BINS, pltpu.roll(later, BINS - 1, 0), END)
    for s in (1, 2, 4, 8, 16):
        ahead = pltpu.roll(later, BINS - s, 0)
        later = jnp.minimum(later, jnp.where(row + s < BINS, ahead, END))
    live = jnp.sum(jnp.where(weight > 0.0, 1.0, 0.0), axis=1, keepdims=True)
    live = jnp.broadcast_to(jnp.sum(live, axis=0, keepdims=True), (8, 128)).astype(jnp.int32)
    tail, _ = iotas(8)
    tail = jnp.where(tail == 1, live, END)
    return jnp.concatenate([jnp.minimum(step, later) + PLACES * weight.astype(jnp.int32), tail])


def prologue_kernel(planes, marked, packed, table):
    for c in range(4):
        packed[:BINS, c, :] = planes[c]
    slots = marked.shape[0]
    marked = jnp.transpose(widened(marked[...]))[:BINS]
    row, lane = iotas(BINS)
    candidate = lane.astype(F32)
    counts = jnp.zeros((BINS, 128), F32)
    for k in range(slots):
        counts = counts + jnp.where(marked[:, k : k + 1] == candidate, 1.0, 0.0)
    for n in range(BINS // 4):
        packed[BINS + n] = counts[4 * n : 4 * n + 4]
    inner = jnp.where(lane < BINS, pltpu.roll(counts, 128 - GHOSTS, 1), 0.0)
    mirror = widened(jnp.transpose(inner)[:BINS])
    pairs = jnp.where(lane > row, inner + mirror, 0.0)
    table[...] = table_of(jnp.where(lane == row, 1.0, pairs))


def write_rows(packed, base, left, right, moment):
    span = pl.ds(base, BINS)
    radius = packed[:BINS, 3, :]
    sigma = jnp.sqrt(10.0 * radius)
    one = jnp.ones((BINS, 128), F32)
    zero = jnp.zeros((BINS, 128), F32)
    norm = zero
    for c in range(3):
        place = packed[:BINS, c, :] - 0.5
        norm = norm + place * place
        right[span, c, :] = -2.0 * place
        moment[span, c, :] = sigma * place
        if left is not None:
            left[span, c, :] = place
    moment[span, 3, :] = sigma
    right[span, 3, :] = one
    right[span, 4, :] = norm + 0.0025
    for t in (5, 6, 7):
        right[span, t, :] = zero
    for t in (4, 5, 6, 7):
        moment[span, t, :] = zero
    if left is not None:
        left[span, 3, :] = norm
        left[span, 4, :] = one
        left[span, 5, :] = radius
        left[span, 6, :] = zero
        left[span, 7, :] = zero


def right_operands(n, right, moment, right_b, moment_b):
    high, middle, low = split3(right[n])
    right_b[n] = jnp.concatenate([high, middle, high, middle, low, high]).astype(BF16)
    high, middle, low = split3(moment[n])
    moment_b[n] = jnp.concatenate([high + pltpu.roll(middle, 4, 0), low]).astype(BF16)


def left_operand(n, left):
    high, middle, low = split3(left[n])
    return jnp.transpose(jnp.concatenate([high, high, middle, middle, high, low])).astype(BF16)


def run_tiles(table, target, lt, ra, right, moment, packed_row, acc_a, acc_b, scratch):
    s0, s1, p0, p1 = scratch
    for ref in (s0, s1):
        ref[...] = jnp.ones_like(ref)
    for ref in (p0, p1):
        ref[...] = jnp.zeros_like(ref)

    def bins(f):
        return jnp.minimum(f >> 7, BINS - 1), f & 127

    def times(f):
        return (table[f >> 7, f & 127] >> 13).astype(F32)

    def distances(tiles, s_ref):
        for n, f in enumerate(tiles):
            a, b = bins(f)
            s_ref[n] = jnp.dot(lt[a], right[b], preferred_element_type=F32)

    def weights(tiles, s_ref, p_ref):
        for n, f in enumerate(tiles):
            a, b = bins(f)
            r_b = packed_row(b)
            for g in range(8):
                rows = slice(16 * g, 16 * g + 16)
                s = s_ref[n, rows, :]
                v = jnp.maximum((ra[a, rows, :] + r_b) * lax.rsqrt(s) - 1.0, TINY)
                square = v * v
                w = square * lax.rsqrt(square + v)
                high = w.astype(BF16)
                low = (w - high.astype(F32)).astype(BF16)
                p_ref[n, rows, :128] = high
                p_ref[n, rows, 128:] = low

    def forces(tiles, p_ref):
        for q in range(0, TILES, 2):
            a1, b1 = bins(tiles[q])
            a2, b2 = bins(tiles[q + 1])
            first, second = p_ref[q], p_ref[q + 1]
            scale1, scale2 = times(tiles[q]), times(tiles[q + 1])
            if acc_b is not None:
                c1, c2 = target(a1, b1), target(a2, b2)
                m = jnp.concatenate([moment[a1], moment[a2]], axis=0)
                both = jnp.concatenate(
                    [
                        jnp.concatenate([first[:, :128], second[:, :128]], axis=1),
                        jnp.concatenate([first[:, 128:], second[:, 128:]], axis=1),
                    ],
                    axis=0,
                )
                out = jnp.dot(
                    jnp.concatenate([m, m], axis=1), both, preferred_element_type=F32
                )
                acc_b[c1] += scale1 * out[:16, :128]
                acc_b[c2] += scale2 * out[16:, 128:]
            m = jnp.concatenate([moment[b1], moment[b2]], axis=0)
            out = lax.dot_general(
                jnp.concatenate([m, m], axis=1),
                jnp.concatenate([first, second], axis=0),
                (((1,), (1,)), ((), ())),
                preferred_element_type=F32,
            )
            acc_a[a1] += scale1 * out[:16, :128]
            acc_a[a2] += scale2 * out[16:, 128:]

    def following(f):
        return table[f >> 7, f & 127] & (PLACES - 1)

    def draw(f):
        tiles = []
        for _ in range(TILES):
            tiles.append(f)
            f = following(jnp.minimum(f + 1, END))
        return f, tuple(tiles)

    none = (jnp.int32(END),) * TILES

    def body(_, carry):
        f, second, third = carry
        for half in range(HALVES):
            f, first = draw(f)
            s_from, s_to, p_from, p_to = (s0, s1, p0, p1) if half % 2 == 0 else (s1, s0, p1, p0)
            forces(third, p_from)
            weights(second, s_from, p_to)
            distances(first, s_to)
            second, third = first, second
        return f, second, third

    live = table[BINS + 1, 0]
    halves = (live + TILES - 1) // TILES + 2
    bodies = (halves + HALVES - 1) // HALVES
    lax.fori_loop(0, bodies, body, (following(jnp.int32(0)), none, none))


def own_kernel(table, packed, acc, lt, ra, new_positions, places, sent, left, right, moment, right_b, moment_b, acc_b, *scratch):
    for c in range(3):
        places[c] = packed[:BINS, c, :]
    send = pltpu.make_async_copy(places, new_positions, sent)
    send.start()
    write_rows(packed, 0, left, right, moment)
    depth = lax.broadcasted_iota(jnp.int32, (DEPTH, 128), 0)
    choose = ((depth == 5) | (depth == 21) | (depth == 45)).astype(BF16)

    def turn(n, carry):
        right_operands(n, right, moment, right_b, moment_b)
        columns = left_operand(n, left)
        lt[n] = columns
        ra[n] = jnp.dot(columns, choose, preferred_element_type=F32)
        return carry

    lax.fori_loop(0, BINS, turn, 0, unroll=8)
    acc[...] = jnp.zeros_like(acc)
    acc_b[...] = jnp.zeros_like(acc_b)
    run_tiles(table, lambda a, b: jnp.where(a == b, BINS, b), lt, ra, right_b, moment_b,
              lambda b: packed[b, pl.ds(3, 1), :], acc, acc_b, scratch)
    acc[...] += acc_b[:BINS]
    send.wait()


def cross_kernel(upward, even, odd, packed, velocity, old_force, acc_in, lt, ra,
                 new_velocity, new_force, right, moment, right_b, moment_b, radii, acc,
                 table_v, table, loaded, *scratch):
    is_up = upward[0] > 0
    row, lane = iotas(BINS)

    def counts_of(ref):
        return jnp.concatenate([ref[BINS + n] for n in range(BINS // 4)])

    mine = counts_of(packed)
    lower = jnp.where((lane >= BINS - GHOSTS) & (lane < BINS), pltpu.roll(mine, BINS - GHOSTS, 1), 0.0)
    upper = jnp.where(lane < GHOSTS, pltpu.roll(mine, 128 - BINS - GHOSTS, 1), 0.0)
    blank = jnp.zeros((BINS - GHOSTS, 128), F32)

    def with_partner(counts, above):
        flipped = widened(jnp.transpose(counts))
        above_part = upper + jnp.concatenate([blank, flipped[:GHOSTS]])
        below_part = lower + jnp.concatenate([flipped[BINS + GHOSTS : BINS + 2 * GHOSTS], blank])
        return jnp.where(above, above_part, below_part)

    by_even = with_partner(counts_of(even), is_up)
    by_odd = with_partner(counts_of(odd), jnp.logical_not(is_up))
    table_v[...] = table_of(by_even + pltpu.roll(by_odd, BINS, 1))
    load = pltpu.make_async_copy(table_v, table, loaded)
    load.start()
    write_rows(even, 0, None, right, moment)
    write_rows(odd, BINS, None, right, moment)
    radii[:BINS] = even[:BINS, pl.ds(3, 1), :]
    radii[BINS:] = odd[:BINS, pl.ds(3, 1), :]

    def turn(n, carry):
        right_operands(n, right, moment, right_b, moment_b)
        return carry

    lax.fori_loop(0, 2 * BINS, turn, 0, unroll=8)
    acc[...] = acc_in[...]
    load.wait()
    run_tiles(table, None, lt, ra, right_b, moment_b, lambda b: radii[b], acc, None, scratch)
    radius = packed[:BINS, 3, :]
    sigma = jnp.sqrt(10.0 * radius)
    scale = 1.0 / (125.0 * radius * radius * radius)

    def gathered(c):
        return acc[:, c, :] + acc[:, 4 + c, :] + acc[:, 8 + c, :]

    total = gathered(3)
    for c in range(3):
        force = sigma * ((packed[:BINS, c, :] - 0.5) * total - gathered(c))
        new_force[c] = force
        gravity = -0.5 if c == 1 else 0.0
        accel = (old_force[c] * scale + gravity) + (force * scale + gravity)
        new_velocity[c] = velocity[c] + 0.5 * TIMESTEP * accel


VMEM = pl.BlockSpec(memory_space=pltpu.VMEM)
SMEM = pl.BlockSpec(memory_space=pltpu.SMEM)
HBM = pl.BlockSpec(memory_space=pltpu.HBM)


def pipeline_scratch():
    return [
        pltpu.VMEM((TILES, 128, 128), F32),
        pltpu.VMEM((TILES, 128, 128), F32),
        pltpu.VMEM((TILES, 128, 256), BF16),
        pltpu.VMEM((TILES, 128, 256), BF16),
    ]


def local(positions, radius, velocity, old_force, neighbours, tile_count):
    def by_component(cells):
        return jnp.transpose(cells, (1, 0, 2))

    positions, velocity, old_force = map(by_component, (positions, velocity, old_force))
    cells = jax.ShapeDtypeStruct((3, BINS, 128), F32)
    component = lax.broadcasted_iota(jnp.int32, (4, BINS, 128), 0)
    four = ((0, 1), (0, 0), (0, 0))
    accel = jnp.pad(old_force, four) / (125.0 * radius * radius * radius)[None]
    accel = accel + jnp.where(component == 1, -0.5, 0.0)
    moved = jnp.pad(positions, four) + TIMESTEP * jnp.pad(velocity, four) + 0.5 * TIMESTEP * TIMESTEP * accel
    planes = jnp.where(component < 3, moved, radius[None])
    slot = lax.broadcasted_iota(jnp.int32, (neighbours.shape[1], BINS), 0)
    marked = jnp.where(slot < tile_count[None], neighbours.T, -1).astype(F32)
    packed, own_table = pl.pallas_call(
        prologue_kernel,
        out_shape=(
            jax.ShapeDtypeStruct((BINS + 8, 4, 128), F32),
            jax.ShapeDtypeStruct((BINS + 8, 128), jnp.int32),
        ),
        in_specs=[VMEM] * 2,
        out_specs=(VMEM,) * 2,
        compiler_params=pltpu.CompilerParams(vmem_limit_bytes=8 << 20),
        name="prologue",
    )(planes, marked)

    slabs = lax.axis_size("slab")
    swap_even = [(i + d, i + 1 - d) for i in range(0, slabs - 1, 2) for d in (0, 1)]
    swap_odd = [(i + d, i + 1 - d) for i in range(1, slabs - 1, 2) for d in (0, 1)]
    even = lax.ppermute(packed, "slab", swap_even)
    odd = lax.ppermute(packed, "slab", swap_odd)

    acc, lt, ra, new_positions = pl.pallas_call(
        own_kernel,
        out_shape=(
            jax.ShapeDtypeStruct((BINS, 16, 128), F32),
            jax.ShapeDtypeStruct((BINS, 128, DEPTH), BF16),
            jax.ShapeDtypeStruct((BINS, 128, 128), F32),
            cells,
        ),
        in_specs=[SMEM, VMEM],
        out_specs=(VMEM, VMEM, VMEM, HBM),
        scratch_shapes=[
            pltpu.VMEM((3, BINS, 128), F32),
            pltpu.SemaphoreType.DMA,
            pltpu.VMEM((BINS, 8, 128), F32),
            pltpu.VMEM((BINS, 8, 128), F32),
            pltpu.VMEM((BINS, 8, 128), F32),
            pltpu.VMEM((BINS, DEPTH, 128), BF16),
            pltpu.VMEM((BINS, 16, 128), BF16),
            pltpu.VMEM((BINS + 1, 16, 128), F32),
            *pipeline_scratch(),
        ],
        compiler_params=pltpu.CompilerParams(vmem_limit_bytes=16 << 20),
        cost_estimate=pl.CostEstimate(flops=10**9, bytes_accessed=10**6, transcendentals=0),
        name="own_tiles",
    )(own_table, packed)

    upward = (1 - lax.axis_index("slab") % 2).astype(jnp.int32)[None]
    new_velocity, new_force = pl.pallas_call(
        cross_kernel,
        out_shape=(cells, cells),
        in_specs=[SMEM] + [VMEM] * 8,
        out_specs=(VMEM, VMEM),
        scratch_shapes=[
            pltpu.VMEM((2 * BINS, 8, 128), F32),
            pltpu.VMEM((2 * BINS, 8, 128), F32),
            pltpu.VMEM((2 * BINS, DEPTH, 128), BF16),
            pltpu.VMEM((2 * BINS, 16, 128), BF16),
            pltpu.VMEM((2 * BINS, 1, 128), F32),
            pltpu.VMEM((BINS, 16, 128), F32),
            pltpu.VMEM((BINS + 8, 128), jnp.int32),
            pltpu.SMEM((BINS + 8, 128), jnp.int32),
            pltpu.SemaphoreType.DMA,
            *pipeline_scratch(),
        ],
        compiler_params=pltpu.CompilerParams(vmem_limit_bytes=16 << 20),
        cost_estimate=pl.CostEstimate(flops=10**9, bytes_accessed=10**6, transcendentals=0),
        name="cross_tiles",
    )(upward, even, odd, packed, velocity, old_force, acc, lt, ra)
    return tuple(map(by_component, (new_positions, new_velocity, new_force)))


def solution(mesh):
    flat = P(("slab", "blk"))
    rows = P(("slab", "blk"), None)
    cells = P(("slab", "blk"), None, None)
    return jax.shard_map(
        local,
        mesh=mesh,
        in_specs=(cells, rows, cells, cells, rows, flat),
        out_specs=(cells, cells, cells),
        check_vma=False,
    )
```

```python
import functools

import jax
import jax.numpy as jnp
from jax import lax
from jax.experimental import pallas as pl
from jax.experimental.pallas import tpu as pltpu
from jax.sharding import PartitionSpec as P

GHOSTS = 8
TIMESTEP = 0.2
TINY = 1e-25
TILES = 4
BINS = 32
DEPTH = 48
END = BINS * 128
PLACES = 8192
HALVES = 8
F32 = jnp.float32
BF16 = jnp.bfloat16


def rounded(value):
    return value.astype(BF16).astype(F32)


def split3(value):
    high = rounded(value)
    middle = rounded(value - high)
    return high, middle, value - high - middle


def iotas(rows):
    shape = (rows, 128)
    return lax.broadcasted_iota(jnp.int32, shape, 0), lax.broadcasted_iota(jnp.int32, shape, 1)


def widened(value):
    rows, lanes = value.shape
    return jnp.concatenate([value, jnp.zeros((rows, 128 - lanes), value.dtype)], axis=1)


def table_of(weight):
    row, lane = iotas(BINS)
    step = jnp.where(weight > 0.0, row * 128 + lane, END)
    for s in (1, 2, 4, 8, 16, 32, 64):
        ahead = pltpu.roll(step, 128 - s, 1)
        step = jnp.minimum(step, jnp.where(lane + s < 128, ahead, END))
    later = jnp.broadcast_to(step[:, :1], (BINS, 128))
    later = jnp.where(row + 1 < BINS, pltpu.roll(later, BINS - 1, 0), END)
    for s in (1, 2, 4, 8, 16):
        ahead = pltpu.roll(later, BINS - s, 0)
        later = jnp.minimum(later, jnp.where(row + s < BINS, ahead, END))
    live = jnp.sum(jnp.where(weight > 0.0, 1.0, 0.0), axis=1, keepdims=True)
    live = jnp.broadcast_to(jnp.sum(live, axis=0, keepdims=True), (8, 128)).astype(jnp.int32)
    tail, _ = iotas(8)
    tail = jnp.where(tail == 1, live, END)
    return jnp.concatenate([jnp.minimum(step, later) + PLACES * weight.astype(jnp.int32), tail])


def prologue_kernel(planes, marked, packed, table):
    for c in range(4):
        packed[:BINS, c, :] = planes[c]
    slots = marked.shape[0]
    marked = jnp.transpose(widened(marked[...]))[:BINS]
    row, lane = iotas(BINS)
    candidate = lane.astype(F32)
    counts = jnp.zeros((BINS, 128), F32)
    for k in range(slots):
        counts = counts + jnp.where(marked[:, k : k + 1] == candidate, 1.0, 0.0)
    for n in range(BINS // 4):
        packed[BINS + n] = counts[4 * n : 4 * n + 4]
    inner = jnp.where(lane < BINS, pltpu.roll(counts, 128 - GHOSTS, 1), 0.0)
    mirror = widened(jnp.transpose(inner)[:BINS])
    pairs = jnp.where(lane > row, inner + mirror, 0.0)
    table[...] = table_of(jnp.where(lane == row, 1.0, pairs))


def write_rows(packed, base, left, right, moment):
    span = pl.ds(base, BINS)
    radius = packed[:BINS, 3, :]
    sigma = jnp.sqrt(10.0 * radius)
    one = jnp.ones((BINS, 128), F32)
    zero = jnp.zeros((BINS, 128), F32)
    norm = zero
    for c in range(3):
        place = packed[:BINS, c, :] - 0.5
        norm = norm + place * place
        right[span, c, :] = -2.0 * place
        moment[span, c, :] = sigma * place
        if left is not None:
            left[span, c, :] = place
    moment[span, 3, :] = sigma
    right[span, 3, :] = one
    right[span, 4, :] = norm + 0.0025
    for t in (5, 6, 7):
        right[span, t, :] = zero
    for t in (4, 5, 6, 7):
        moment[span, t, :] = zero
    if left is not None:
        left[span, 3, :] = norm
        left[span, 4, :] = one
        left[span, 5, :] = radius
        left[span, 6, :] = zero
        left[span, 7, :] = zero


def right_operands(n, right, moment, right_b, moment_b):
    high, middle, low = split3(right[n])
    right_b[n] = jnp.concatenate([high, middle, high, middle, low, high]).astype(BF16)
    high, middle, low = split3(moment[n])
    moment_b[n] = jnp.concatenate([high + pltpu.roll(middle, 4, 0), low]).astype(BF16)


def left_operand(n, left):
    high, middle, low = split3(left[n])
    return jnp.transpose(jnp.concatenate([high, high, middle, middle, high, low])).astype(BF16)


def run_tiles(table, target, lt, ra, right, moment, packed_row, acc_a, acc_b, scratch):
    s0, s1, p0, p1 = scratch
    s0[...] = jnp.ones_like(s0)
    p0[...] = jnp.zeros_like(p0)

    def bins(f):
        return jnp.minimum(f >> 7, BINS - 1), f & 127

    def times(f):
        return (table[f >> 7, f & 127] >> 13).astype(F32)

    def distances(tiles, s_ref):
        for n, f in enumerate(tiles):
            a, b = bins(f)
            s_ref[n] = jnp.dot(lt[a], right[b], preferred_element_type=F32)

    def weights(tiles, s_ref, p_ref):
        for n, f in enumerate(tiles):
            a, b = bins(f)
            r_b = packed_row(b)
            for g in range(8):
                rows = slice(16 * g, 16 * g + 16)
                s = s_ref[n, rows, :]
                v = jnp.maximum((ra[a, rows, :] + r_b) * lax.rsqrt(s) - 1.0, TINY)
                square = v * v
                w = square * lax.rsqrt(square + v)
                high = w.astype(BF16)
                low = (w - high.astype(F32)).astype(BF16)
                p_ref[n, rows, :128] = high
                p_ref[n, rows, 128:] = low

    def forces(tiles, p_ref):
        for q in range(0, TILES, 2):
            a1, b1 = bins(tiles[q])
            a2, b2 = bins(tiles[q + 1])
            first, second = p_ref[q], p_ref[q + 1]
            scale1, scale2 = times(tiles[q]), times(tiles[q + 1])
            if acc_b is not None:
                c1, c2 = target(a1, b1), target(a2, b2)
                m = jnp.concatenate([moment[a1], moment[a2]], axis=0)
                both = jnp.concatenate(
                    [
                        jnp.concatenate([first[:, :128], second[:, :128]], axis=1),
                        jnp.concatenate([first[:, 128:], second[:, 128:]], axis=1),
                    ],
                    axis=0,
                )
                out = jnp.dot(
                    jnp.concatenate([m, m], axis=1), both, preferred_element_type=F32
                )
                acc_b[c1] += scale1 * out[:16, :128]
                acc_b[c2] += scale2 * out[16:, 128:]
            m = jnp.concatenate([moment[b1], moment[b2]], axis=0)
            out = lax.dot_general(
                jnp.concatenate([m, m], axis=1),
                jnp.concatenate([first, second], axis=0),
                (((1,), (1,)), ((), ())),
                preferred_element_type=F32,
            )
            acc_a[a1] += scale1 * out[:16, :128]
            acc_a[a2] += scale2 * out[16:, 128:]

    def following(f):
        return table[f >> 7, f & 127] & (PLACES - 1)

    def draw(f):
        tiles = []
        for _ in range(TILES):
            tiles.append(f)
            f = following(jnp.minimum(f + 1, END))
        return f, tuple(tiles)

    none = (jnp.int32(END),) * TILES

    def body(count, _, carry):
        f, second, third = carry
        for half in range(count):
            f, first = draw(f)
            s_from, s_to, p_from, p_to = (s0, s1, p0, p1) if half % 2 == 0 else (s1, s0, p1, p0)
            forces(third, p_from)
            weights(second, s_from, p_to)
            distances(first, s_to)
            second, third = first, second
        return f, second, third

    live = table[BINS + 1, 0]
    halves = (live + TILES - 1) // TILES + 2
    long = halves // HALVES
    short = (halves - long * HALVES + 1) // 2
    carry = (following(jnp.int32(0)), none, none)
    carry = lax.fori_loop(0, long, functools.partial(body, HALVES), carry)
    lax.fori_loop(0, short, functools.partial(body, 2), carry)


def own_kernel(table_v, packed, acc, lt, ra, new_positions, places, sent, table, loaded, left, right, moment, right_b, moment_b, acc_b, *scratch):
    load = pltpu.make_async_copy(table_v, table, loaded)
    load.start()
    for c in range(3):
        places[c] = packed[:BINS, c, :]
    send = pltpu.make_async_copy(places, new_positions, sent)
    send.start()
    write_rows(packed, 0, left, right, moment)
    depth = lax.broadcasted_iota(jnp.int32, (DEPTH, 128), 0)
    choose = ((depth == 5) | (depth == 21) | (depth == 45)).astype(BF16)

    def turn(n, carry):
        right_operands(n, right, moment, right_b, moment_b)
        columns = left_operand(n, left)
        lt[n] = columns
        ra[n] = jnp.dot(columns, choose, preferred_element_type=F32)
        return carry

    lax.fori_loop(0, BINS, turn, 0, unroll=8)
    acc[...] = jnp.zeros_like(acc)
    acc_b[...] = jnp.zeros_like(acc_b)
    load.wait()
    run_tiles(table, lambda a, b: jnp.where(a == b, BINS, b), lt, ra, right_b, moment_b,
              lambda b: packed[b, pl.ds(3, 1), :], acc, acc_b, scratch)
    acc[...] += acc_b[:BINS]
    send.wait()


def cross_kernel(upward, even, odd, packed, velocity, old_force, acc_in, lt, ra,
                 new_velocity, new_force, right, moment, right_b, moment_b, radii, acc,
                 table_v, table, loaded, *scratch):
    is_up = upward[0] > 0
    row, lane = iotas(BINS)

    def counts_of(ref):
        return jnp.concatenate([ref[BINS + n] for n in range(BINS // 4)])

    mine = counts_of(packed)
    lower = jnp.where((lane >= BINS - GHOSTS) & (lane < BINS), pltpu.roll(mine, BINS - GHOSTS, 1), 0.0)
    upper = jnp.where(lane < GHOSTS, pltpu.roll(mine, 128 - BINS - GHOSTS, 1), 0.0)
    blank = jnp.zeros((BINS - GHOSTS, 128), F32)

    def with_partner(counts, above):
        flipped = widened(jnp.transpose(counts))
        above_part = upper + jnp.concatenate([blank, flipped[:GHOSTS]])
        below_part = lower + jnp.concatenate([flipped[BINS + GHOSTS : BINS + 2 * GHOSTS], blank])
        return jnp.where(above, above_part, below_part)

    by_even = with_partner(counts_of(even), is_up)
    by_odd = with_partner(counts_of(odd), jnp.logical_not(is_up))
    table_v[...] = table_of(by_even + pltpu.roll(by_odd, BINS, 1))
    load = pltpu.make_async_copy(table_v, table, loaded)
    load.start()
    write_rows(even, 0, None, right, moment)
    write_rows(odd, BINS, None, right, moment)
    radii[:BINS] = even[:BINS, pl.ds(3, 1), :]
    radii[BINS:] = odd[:BINS, pl.ds(3, 1), :]

    def turn(n, carry):
        right_operands(n, right, moment, right_b, moment_b)
        return carry

    lax.fori_loop(0, 2 * BINS, turn, 0, unroll=8)
    acc[...] = acc_in[...]
    load.wait()
    run_tiles(table, None, lt, ra, right_b, moment_b, lambda b: radii[b], acc, None, scratch)
    radius = packed[:BINS, 3, :]
    sigma = jnp.sqrt(10.0 * radius)
    scale = 1.0 / (125.0 * radius * radius * radius)

    def gathered(c):
        return acc[:, c, :] + acc[:, 4 + c, :] + acc[:, 8 + c, :]

    total = gathered(3)
    for c in range(3):
        force = sigma * ((packed[:BINS, c, :] - 0.5) * total - gathered(c))
        new_force[c] = force
        gravity = -0.5 if c == 1 else 0.0
        accel = (old_force[c] * scale + gravity) + (force * scale + gravity)
        new_velocity[c] = velocity[c] + 0.5 * TIMESTEP * accel


VMEM = pl.BlockSpec(memory_space=pltpu.VMEM)
SMEM = pl.BlockSpec(memory_space=pltpu.SMEM)
HBM = pl.BlockSpec(memory_space=pltpu.HBM)


def pipeline_scratch():
    return [
        pltpu.VMEM((TILES, 128, 128), F32),
        pltpu.VMEM((TILES, 128, 128), F32),
        pltpu.VMEM((TILES, 128, 256), BF16),
        pltpu.VMEM((TILES, 128, 256), BF16),
    ]


def local(positions, radius, velocity, old_force, neighbours, tile_count):
    def by_component(cells):
        return jnp.transpose(cells, (1, 0, 2))

    positions, velocity, old_force = map(by_component, (positions, velocity, old_force))
    cells = jax.ShapeDtypeStruct((3, BINS, 128), F32)
    slot = lax.broadcasted_iota(jnp.int32, (neighbours.shape[1], BINS), 0)
    marked = jnp.where(slot < tile_count[None], neighbours.T, -1).astype(F32)
    component = lax.broadcasted_iota(jnp.int32, (4, BINS, 128), 0)
    four = ((0, 1), (0, 0), (0, 0))
    each_radius = jnp.where(component < 3, radius[None], 1.0)
    accel = jnp.pad(old_force, four) / (125.0 * each_radius * each_radius * each_radius)
    accel = accel + jnp.where(component == 1, -0.5, 0.0)
    moved = jnp.pad(positions, four) + TIMESTEP * jnp.pad(velocity, four) + 0.5 * TIMESTEP * TIMESTEP * accel
    planes = jnp.where(component < 3, moved, radius[None])
    packed, own_table = pl.pallas_call(
        prologue_kernel,
        out_shape=(
            jax.ShapeDtypeStruct((BINS + 8, 4, 128), F32),
            jax.ShapeDtypeStruct((BINS + 8, 128), jnp.int32),
        ),
        in_specs=[VMEM] * 2,
        out_specs=(VMEM,) * 2,
        compiler_params=pltpu.CompilerParams(vmem_limit_bytes=8 << 20),
        name="prologue",
    )(planes, marked)

    slabs = lax.axis_size("slab")
    swap_even = [(i + d, i + 1 - d) for i in range(0, slabs - 1, 2) for d in (0, 1)]
    swap_odd = [(i + d, i + 1 - d) for i in range(1, slabs - 1, 2) for d in (0, 1)]
    even = lax.ppermute(packed, "slab", swap_even)
    odd = lax.ppermute(packed, "slab", swap_odd)

    acc, lt, ra, new_positions = pl.pallas_call(
        own_kernel,
        out_shape=(
            jax.ShapeDtypeStruct((BINS, 16, 128), F32),
            jax.ShapeDtypeStruct((BINS, 128, DEPTH), BF16),
            jax.ShapeDtypeStruct((BINS, 128, 128), F32),
            cells,
        ),
        in_specs=[VMEM, VMEM],
        out_specs=(VMEM, VMEM, VMEM, HBM),
        scratch_shapes=[
            pltpu.VMEM((3, BINS, 128), F32),
            pltpu.SemaphoreType.DMA,
            pltpu.SMEM((BINS + 8, 128), jnp.int32),
            pltpu.SemaphoreType.DMA,
            pltpu.VMEM((BINS, 8, 128), F32),
            pltpu.VMEM((BINS, 8, 128), F32),
            pltpu.VMEM((BINS, 8, 128), F32),
            pltpu.VMEM((BINS, DEPTH, 128), BF16),
            pltpu.VMEM((BINS, 16, 128), BF16),
            pltpu.VMEM((BINS + 1, 16, 128), F32),
            *pipeline_scratch(),
        ],
        compiler_params=pltpu.CompilerParams(vmem_limit_bytes=16 << 20),
        cost_estimate=pl.CostEstimate(flops=10**9, bytes_accessed=10**6, transcendentals=0),
        name="own_tiles",
    )(own_table, packed)

    upward = (1 - lax.axis_index("slab") % 2).astype(jnp.int32)[None]
    new_velocity, new_force = pl.pallas_call(
        cross_kernel,
        out_shape=(cells, cells),
        in_specs=[SMEM] + [VMEM] * 8,
        out_specs=(VMEM, VMEM),
        scratch_shapes=[
            pltpu.VMEM((2 * BINS, 8, 128), F32),
            pltpu.VMEM((2 * BINS, 8, 128), F32),
            pltpu.VMEM((2 * BINS, DEPTH, 128), BF16),
            pltpu.VMEM((2 * BINS, 16, 128), BF16),
            pltpu.VMEM((2 * BINS, 1, 128), F32),
            pltpu.VMEM((BINS, 16, 128), F32),
            pltpu.VMEM((BINS + 8, 128), jnp.int32),
            pltpu.SMEM((BINS + 8, 128), jnp.int32),
            pltpu.SemaphoreType.DMA,
            *pipeline_scratch(),
        ],
        compiler_params=pltpu.CompilerParams(vmem_limit_bytes=16 << 20),
        cost_estimate=pl.CostEstimate(flops=10**9, bytes_accessed=10**6, transcendentals=0),
        name="cross_tiles",
    )(upward, even, odd, packed, velocity, old_force, acc, lt, ra)
    return tuple(map(by_component, (new_positions, new_velocity, new_force)))


def solution(mesh):
    flat = P(("slab", "blk"))
    rows = P(("slab", "blk"), None)
    cells = P(("slab", "blk"), None, None)
    return jax.shard_map(
        local,
        mesh=mesh,
        in_specs=(cells, rows, cells, cells, rows, flat),
        out_specs=(cells, cells, cells),
        check_vma=False,
    )
```

```python
import functools

import jax
import jax.numpy as jnp
from jax import lax
from jax.experimental import pallas as pl
from jax.experimental.pallas import tpu as pltpu
from jax.sharding import PartitionSpec as P

GHOSTS = 8
TIMESTEP = 0.2
TINY = 1e-25
TILES = 4
BINS = 32
DEPTH = 48
END = BINS * 128
PLACES = 8192
HALVES = 8
F32 = jnp.float32
BF16 = jnp.bfloat16


def rounded(value):
    return value.astype(BF16).astype(F32)


def split3(value):
    high = rounded(value)
    middle = rounded(value - high)
    return high, middle, value - high - middle


def iotas(rows):
    shape = (rows, 128)
    return lax.broadcasted_iota(jnp.int32, shape, 0), lax.broadcasted_iota(jnp.int32, shape, 1)


def widened(value):
    rows, lanes = value.shape
    return jnp.concatenate([value, jnp.zeros((rows, 128 - lanes), value.dtype)], axis=1)


def table_of(weight, span):
    row, lane = iotas(BINS)
    step = jnp.where(weight > 0.0, row * 128 + lane, END)
    for s in (1, 2, 4, 8, 16, 32)[:span]:
        ahead = pltpu.roll(step, 128 - s, 1)
        step = jnp.minimum(step, jnp.where(lane + s < 128, ahead, END))
    later = jnp.broadcast_to(step[:, :1], (BINS, 128))
    later = jnp.where(row + 1 < BINS, pltpu.roll(later, BINS - 1, 0), END)
    for s in (1, 2, 4, 8, 16):
        ahead = pltpu.roll(later, BINS - s, 0)
        later = jnp.minimum(later, jnp.where(row + s < BINS, ahead, END))
    live = jnp.sum(jnp.where(weight > 0.0, 1.0, 0.0), axis=1, keepdims=True)
    live = jnp.broadcast_to(jnp.sum(live, axis=0, keepdims=True), (8, 128)).astype(jnp.int32)
    tail, _ = iotas(8)
    tail = jnp.where(tail == 1, live, END)
    return jnp.concatenate([jnp.minimum(step, later) + PLACES * weight.astype(jnp.int32), tail])


def prologue_kernel(slots, planes, packed, table):
    for c in range(4):
        packed[:BINS, c, :] = planes[c]
    slot = lax.broadcasted_iota(jnp.int32, (slots, 128), 0).astype(F32)
    marked = jnp.where(slot < planes[4, pl.ds(BINS - 1, 1), :], planes[4, :slots, :], -1.0)
    marked = jnp.transpose(marked)[:BINS]
    row, lane = iotas(BINS)
    candidate = lane.astype(F32)
    counts = jnp.zeros((BINS, 128), F32)
    for k in range(slots):
        counts = counts + jnp.where(marked[:, k : k + 1] == candidate, 1.0, 0.0)
    for n in range(BINS // 4):
        packed[BINS + n] = counts[4 * n : 4 * n + 4]
    inner = jnp.where(lane < BINS, pltpu.roll(counts, 128 - GHOSTS, 1), 0.0)
    mirror = widened(jnp.transpose(inner)[:BINS])
    pairs = jnp.where(lane > row, inner + mirror, 0.0)
    table[...] = table_of(jnp.where(lane == row, 1.0, pairs), 5)


def write_rows(packed, base, left, right, moment):
    span = pl.ds(base, BINS)
    radius = packed[:BINS, 3, :]
    sigma = jnp.sqrt(10.0 * radius)
    one = jnp.ones((BINS, 128), F32)
    zero = jnp.zeros((BINS, 128), F32)
    norm = zero
    for c in range(3):
        place = packed[:BINS, c, :] - 0.5
        norm = norm + place * place
        right[span, c, :] = -2.0 * place
        moment[span, c, :] = sigma * place
        if left is not None:
            left[span, c, :] = place
    moment[span, 3, :] = sigma
    right[span, 3, :] = one
    right[span, 4, :] = norm + 0.0025
    for t in (5, 6, 7):
        right[span, t, :] = zero
    for t in (4, 5, 6, 7):
        moment[span, t, :] = zero
    if left is not None:
        left[span, 3, :] = norm
        left[span, 4, :] = one
        left[span, 5, :] = radius
        left[span, 6, :] = zero
        left[span, 7, :] = zero


def right_operands(n, right, moment, right_b, moment_b):
    high, middle, low = split3(right[n])
    right_b[n] = jnp.concatenate([high, middle, high, middle, low, high]).astype(BF16)
    high, middle, low = split3(moment[n])
    moment_b[n] = jnp.concatenate([high + pltpu.roll(middle, 4, 0), low]).astype(BF16)


def left_operand(n, left):
    high, middle, low = split3(left[n])
    return jnp.transpose(jnp.concatenate([high, high, middle, middle, high, low])).astype(BF16)


def run_tiles(table, target, lt, ra, right, moment, packed_row, acc_a, acc_b, scratch):
    s0, s1, p0, p1 = scratch
    s0[...] = jnp.ones_like(s0)
    p0[...] = jnp.zeros_like(p0)

    def bins(f):
        return jnp.minimum(f >> 7, BINS - 1), f & 127

    def times(f):
        return (table[f >> 7, f & 127] >> 13).astype(F32)

    def distances(tiles, s_ref):
        for n, f in enumerate(tiles):
            a, b = bins(f)
            s_ref[n] = jnp.dot(lt[a], right[b], preferred_element_type=F32)

    def weights(tiles, s_ref, p_ref):
        for n, f in enumerate(tiles):
            a, b = bins(f)
            r_b = packed_row(b)
            for g in range(8):
                rows = slice(16 * g, 16 * g + 16)
                s = s_ref[n, rows, :]
                v = jnp.maximum((ra[a, rows, :] + r_b) * lax.rsqrt(s) - 1.0, TINY)
                square = v * v
                w = square * lax.rsqrt(square + v)
                high = w.astype(BF16)
                low = (w - high.astype(F32)).astype(BF16)
                p_ref[n, 0, rows, :] = high
                p_ref[n, 1, rows, :] = low

    def forces(tiles, p_ref):
        for q in range(0, TILES, 2):
            a1, b1 = bins(tiles[q])
            a2, b2 = bins(tiles[q + 1])
            high1, low1 = p_ref[q, 0], p_ref[q, 1]
            high2, low2 = p_ref[q + 1, 0], p_ref[q + 1, 1]
            scale1, scale2 = times(tiles[q]), times(tiles[q + 1])
            if acc_b is not None:
                c1, c2 = target(a1, b1), target(a2, b2)
                m = jnp.concatenate([moment[a1], moment[a2]], axis=0)
                both = jnp.concatenate(
                    [
                        jnp.concatenate([high1, high2], axis=1),
                        jnp.concatenate([low1, low2], axis=1),
                    ],
                    axis=0,
                )
                out = jnp.dot(
                    jnp.concatenate([m, m], axis=1), both, preferred_element_type=F32
                )
                acc_b[c1] += scale1 * out[:16, :128]
                acc_b[c2] += scale2 * out[16:, 128:]
            m = jnp.concatenate([moment[b1], moment[b2]], axis=0)
            out = lax.dot_general(
                jnp.concatenate([m, m], axis=1),
                jnp.concatenate(
                    [
                        jnp.concatenate([high1, low1], axis=1),
                        jnp.concatenate([high2, low2], axis=1),
                    ],
                    axis=0,
                ),
                (((1,), (1,)), ((), ())),
                preferred_element_type=F32,
            )
            acc_a[a1] += scale1 * out[:16, :128]
            acc_a[a2] += scale2 * out[16:, 128:]

    def following(f):
        return table[f >> 7, f & 127] & (PLACES - 1)

    def draw(f):
        tiles = []
        for _ in range(TILES):
            tiles.append(f)
            f = following(jnp.minimum(f + 1, END))
        return f, tuple(tiles)

    none = (jnp.int32(END),) * TILES

    def body(count, _, carry):
        f, second, third = carry
        for half in range(count):
            f, first = draw(f)
            s_from, s_to, p_from, p_to = (s0, s1, p0, p1) if half % 2 == 0 else (s1, s0, p1, p0)
            forces(third, p_from)
            weights(second, s_from, p_to)
            distances(first, s_to)
            second, third = first, second
        return f, second, third

    live = table[BINS + 1, 0]
    halves = (live + TILES - 1) // TILES + 2
    long = halves // HALVES
    short = (halves - long * HALVES + 1) // 2
    carry = (following(jnp.int32(0)), none, none)
    carry = lax.fori_loop(0, long, functools.partial(body, HALVES), carry)
    lax.fori_loop(0, short, functools.partial(body, 2), carry)


def own_kernel(table_v, packed, acc, lt, ra, new_positions, places, sent, table, loaded, left, right, moment, right_b, moment_b, acc_b, *scratch):
    load = pltpu.make_async_copy(table_v, table, loaded)
    load.start()
    for c in range(3):
        places[c] = packed[:BINS, c, :]
    send = pltpu.make_async_copy(places, new_positions, sent)
    send.start()
    write_rows(packed, 0, left, right, moment)
    depth = lax.broadcasted_iota(jnp.int32, (DEPTH, 128), 0)
    choose = ((depth == 5) | (depth == 21) | (depth == 45)).astype(BF16)

    def turn(n, carry):
        right_operands(n, right, moment, right_b, moment_b)
        columns = left_operand(n, left)
        lt[n] = columns
        ra[n] = jnp.dot(columns, choose, preferred_element_type=F32)
        return carry

    lax.fori_loop(0, BINS, turn, 0, unroll=8)
    acc[...] = jnp.zeros_like(acc)
    acc_b[...] = jnp.zeros_like(acc_b)
    load.wait()
    run_tiles(table, lambda a, b: jnp.where(a == b, BINS, b), lt, ra, right_b, moment_b,
              lambda b: packed[b, pl.ds(3, 1), :], acc, acc_b, scratch)
    acc[...] += acc_b[:BINS]
    send.wait()


def cross_kernel(upward, even, odd, packed, velocity, old_force, acc_in, lt, ra,
                 new_velocity, new_force, right, moment, right_b, moment_b, radii, acc,
                 table_v, table, loaded, *scratch):
    is_up = upward[0] > 0
    row, lane = iotas(BINS)

    def counts_of(ref):
        return jnp.concatenate([ref[BINS + n] for n in range(BINS // 4)])

    mine = counts_of(packed)
    lower = jnp.where((lane >= BINS - GHOSTS) & (lane < BINS), pltpu.roll(mine, BINS - GHOSTS, 1), 0.0)
    upper = jnp.where(lane < GHOSTS, pltpu.roll(mine, 128 - BINS - GHOSTS, 1), 0.0)
    blank = jnp.zeros((BINS - GHOSTS, 128), F32)

    def with_partner(counts, above):
        flipped = widened(jnp.transpose(counts))
        above_part = upper + jnp.concatenate([blank, flipped[:GHOSTS]])
        below_part = lower + jnp.concatenate([flipped[BINS + GHOSTS : BINS + 2 * GHOSTS], blank])
        return jnp.where(above, above_part, below_part)

    by_even = with_partner(counts_of(even), is_up)
    by_odd = with_partner(counts_of(odd), jnp.logical_not(is_up))
    table_v[...] = table_of(by_even + pltpu.roll(by_odd, BINS, 1), 6)
    load = pltpu.make_async_copy(table_v, table, loaded)
    load.start()
    write_rows(even, 0, None, right, moment)
    write_rows(odd, BINS, None, right, moment)
    radii[:BINS] = even[:BINS, pl.ds(3, 1), :]
    radii[BINS:] = odd[:BINS, pl.ds(3, 1), :]

    def turn(n, carry):
        right_operands(n, right, moment, right_b, moment_b)
        return carry

    lax.fori_loop(0, 2 * BINS, turn, 0, unroll=8)
    acc[...] = acc_in[...]
    load.wait()
    run_tiles(table, None, lt, ra, right_b, moment_b, lambda b: radii[b], acc, None, scratch)
    radius = packed[:BINS, 3, :]
    sigma = jnp.sqrt(10.0 * radius)
    scale = 1.0 / (125.0 * radius * radius * radius)

    def gathered(c):
        return acc[:, c, :] + acc[:, 4 + c, :] + acc[:, 8 + c, :]

    total = gathered(3)
    for c in range(3):
        force = sigma * ((packed[:BINS, c, :] - 0.5) * total - gathered(c))
        new_force[c] = force
        gravity = -0.5 if c == 1 else 0.0
        accel = (old_force[c] * scale + gravity) + (force * scale + gravity)
        new_velocity[c] = velocity[c] + 0.5 * TIMESTEP * accel


VMEM = pl.BlockSpec(memory_space=pltpu.VMEM)
SMEM = pl.BlockSpec(memory_space=pltpu.SMEM)
HBM = pl.BlockSpec(memory_space=pltpu.HBM)


def pipeline_scratch():
    return [
        pltpu.VMEM((TILES, 128, 128), F32),
        pltpu.VMEM((TILES, 128, 128), F32),
        pltpu.VMEM((TILES, 2, 128, 128), BF16),
        pltpu.VMEM((TILES, 2, 128, 128), BF16),
    ]


def local(positions, radius, velocity, old_force, neighbours, tile_count):
    def by_component(cells):
        return jnp.transpose(cells, (1, 0, 2))

    positions, velocity, old_force = map(by_component, (positions, velocity, old_force))
    cells = jax.ShapeDtypeStruct((3, BINS, 128), F32)
    slots = neighbours.shape[1]
    component = lax.broadcasted_iota(jnp.int32, (5, BINS, 128), 0)
    five = ((0, 2), (0, 0), (0, 0))
    each_radius = jnp.where(component < 3, radius[None], 1.0)
    accel = jnp.pad(old_force, five) / (125.0 * each_radius * each_radius * each_radius)
    accel = accel + jnp.where(component == 1, -0.5, 0.0)
    moved = jnp.pad(positions, five) + TIMESTEP * jnp.pad(velocity, five) + 0.5 * TIMESTEP * TIMESTEP * accel
    planes = jnp.where(component < 3, moved, radius[None])
    listed = jnp.pad(neighbours.T[None], ((4, 0), (0, BINS - slots), (0, 128 - BINS)))
    counted = jnp.pad(tile_count[None, None], ((4, 0), (BINS - 1, 0), (0, 128 - BINS)))
    planes = jnp.where(component < 4, planes, (listed + counted).astype(F32))
    packed, own_table = pl.pallas_call(
        functools.partial(prologue_kernel, slots),
        out_shape=(
            jax.ShapeDtypeStruct((BINS + 8, 4, 128), F32),
            jax.ShapeDtypeStruct((BINS + 8, 128), jnp.int32),
        ),
        in_specs=[VMEM],
        out_specs=(VMEM,) * 2,
        compiler_params=pltpu.CompilerParams(vmem_limit_bytes=8 << 20),
        name="prologue",
    )(planes)

    slabs = lax.axis_size("slab")
    swap_even = [(i + d, i + 1 - d) for i in range(0, slabs - 1, 2) for d in (0, 1)]
    swap_odd = [(i + d, i + 1 - d) for i in range(1, slabs - 1, 2) for d in (0, 1)]
    even = lax.ppermute(packed, "slab", swap_even)
    odd = lax.ppermute(packed, "slab", swap_odd)

    acc, lt, ra, new_positions = pl.pallas_call(
        own_kernel,
        out_shape=(
            jax.ShapeDtypeStruct((BINS, 16, 128), F32),
            jax.ShapeDtypeStruct((BINS, 128, DEPTH), BF16),
            jax.ShapeDtypeStruct((BINS, 128, 128), F32),
            cells,
        ),
        in_specs=[VMEM, VMEM],
        out_specs=(VMEM, VMEM, VMEM, HBM),
        scratch_shapes=[
            pltpu.VMEM((3, BINS, 128), F32),
            pltpu.SemaphoreType.DMA,
            pltpu.SMEM((BINS + 8, 128), jnp.int32),
            pltpu.SemaphoreType.DMA,
            pltpu.VMEM((BINS, 8, 128), F32),
            pltpu.VMEM((BINS, 8, 128), F32),
            pltpu.VMEM((BINS, 8, 128), F32),
            pltpu.VMEM((BINS, DEPTH, 128), BF16),
            pltpu.VMEM((BINS, 16, 128), BF16),
            pltpu.VMEM((BINS + 1, 16, 128), F32),
            *pipeline_scratch(),
        ],
        compiler_params=pltpu.CompilerParams(vmem_limit_bytes=16 << 20),
        cost_estimate=pl.CostEstimate(flops=10**9, bytes_accessed=10**6, transcendentals=0),
        name="own_tiles",
    )(own_table, packed)

    upward = (1 - lax.axis_index("slab") % 2).astype(jnp.int32)[None]
    new_velocity, new_force = pl.pallas_call(
        cross_kernel,
        out_shape=(cells, cells),
        in_specs=[SMEM] + [VMEM] * 8,
        out_specs=(VMEM, VMEM),
        scratch_shapes=[
            pltpu.VMEM((2 * BINS, 8, 128), F32),
            pltpu.VMEM((2 * BINS, 8, 128), F32),
            pltpu.VMEM((2 * BINS, DEPTH, 128), BF16),
            pltpu.VMEM((2 * BINS, 16, 128), BF16),
            pltpu.VMEM((2 * BINS, 1, 128), F32),
            pltpu.VMEM((BINS, 16, 128), F32),
            pltpu.VMEM((BINS + 8, 128), jnp.int32),
            pltpu.SMEM((BINS + 8, 128), jnp.int32),
            pltpu.SemaphoreType.DMA,
            *pipeline_scratch(),
        ],
        compiler_params=pltpu.CompilerParams(vmem_limit_bytes=16 << 20),
        cost_estimate=pl.CostEstimate(flops=10**9, bytes_accessed=10**6, transcendentals=0),
        name="cross_tiles",
    )(upward, even, odd, packed, velocity, old_force, acc, lt, ra)
    return tuple(map(by_component, (new_positions, new_velocity, new_force)))


def solution(mesh):
    flat = P(("slab", "blk"))
    rows = P(("slab", "blk"), None)
    cells = P(("slab", "blk"), None, None)
    return jax.shard_map(
        local,
        mesh=mesh,
        in_specs=(cells, rows, cells, cells, rows, flat),
        out_specs=(cells, cells, cells),
        check_vma=False,
    )
```

```python
import functools

import jax
import jax.numpy as jnp
from jax import lax
from jax.experimental import pallas as pl
from jax.experimental.pallas import tpu as pltpu
from jax.sharding import PartitionSpec as P

GHOSTS = 8
TIMESTEP = 0.2
TINY = 1e-25
TILES = 4
BINS = 32
DEPTH = 48
END = BINS * 128
PLACES = 8192
HALVES = 8
F32 = jnp.float32
BF16 = jnp.bfloat16


def rounded(value):
    return value.astype(BF16).astype(F32)


def split3(value):
    high = rounded(value)
    middle = rounded(value - high)
    return high, middle, value - high - middle


def iotas(rows):
    shape = (rows, 128)
    return lax.broadcasted_iota(jnp.int32, shape, 0), lax.broadcasted_iota(jnp.int32, shape, 1)


def widened(value):
    rows, lanes = value.shape
    return jnp.concatenate([value, jnp.zeros((rows, 128 - lanes), value.dtype)], axis=1)


def table_of(weight, span):
    row, lane = iotas(BINS)
    step = jnp.where(weight > 0.0, row * 128 + lane, END)
    for s in (1, 2, 4, 8, 16, 32)[:span]:
        ahead = pltpu.roll(step, 128 - s, 1)
        step = jnp.minimum(step, jnp.where(lane + s < 128, ahead, END))
    later = jnp.broadcast_to(step[:, :1], (BINS, 128))
    later = jnp.where(row + 1 < BINS, pltpu.roll(later, BINS - 1, 0), END)
    for s in (1, 2, 4, 8, 16):
        ahead = pltpu.roll(later, BINS - s, 0)
        later = jnp.minimum(later, jnp.where(row + s < BINS, ahead, END))
    live = jnp.sum(jnp.where(weight > 0.0, 1.0, 0.0), axis=1, keepdims=True)
    live = jnp.broadcast_to(jnp.sum(live, axis=0, keepdims=True), (8, 128)).astype(jnp.int32)
    tail, _ = iotas(8)
    tail = jnp.where(tail == 1, live, END)
    return jnp.concatenate([jnp.minimum(step, later) + PLACES * weight.astype(jnp.int32), tail])


def prologue_kernel(slots, planes, packed, table):
    for c in range(4):
        packed[:BINS, c, :] = planes[c]
    slot = lax.broadcasted_iota(jnp.int32, (slots, 128), 0).astype(F32)
    marked = jnp.where(slot < planes[4, pl.ds(BINS - 1, 1), :], planes[4, :slots, :], -1.0)
    marked = jnp.transpose(marked)[:BINS]
    row, lane = iotas(BINS)
    candidate = lane.astype(F32)
    counts = jnp.zeros((BINS, 128), F32)
    for k in range(slots):
        counts = counts + jnp.where(marked[:, k : k + 1] == candidate, 1.0, 0.0)
    for n in range(BINS // 4):
        packed[BINS + n] = counts[4 * n : 4 * n + 4]
    inner = jnp.where(lane < BINS, pltpu.roll(counts, 128 - GHOSTS, 1), 0.0)
    mirror = widened(jnp.transpose(inner)[:BINS])
    pairs = jnp.where(lane > row, inner + mirror, 0.0)
    table[...] = table_of(jnp.where(lane == row, 1.0, pairs), 5)


def bin_rows(cell):
    cell = jnp.concatenate([cell, jnp.zeros((4, 128), F32)])
    row = lax.broadcasted_iota(jnp.int32, (8, 128), 0)
    radius = cell[3:4]
    sigma = jnp.sqrt(10.0 * radius)
    place = jnp.where(row < 3, cell - 0.5, 0.0)
    square = place * place
    norm = square[0:1] + square[1:2] + square[2:3]
    right = jnp.where(row == 3, 1.0, jnp.where(row == 4, norm + 0.0025, -2.0 * place))
    left = jnp.where(row == 3, norm, jnp.where(row == 4, 1.0, jnp.where(row == 5, radius, place)))
    moment = sigma * jnp.where(row == 3, 1.0, place)
    return right, left, moment


def right_operand(rows):
    high, middle, low = split3(rows)
    return jnp.concatenate([high, middle, high, middle, low, high]).astype(BF16)


def left_operand(rows):
    high, middle, low = split3(rows)
    return jnp.transpose(jnp.concatenate([high, high, middle, middle, high, low])).astype(BF16)


def moment_operand(rows):
    high, middle, low = split3(rows)
    return jnp.concatenate([high + pltpu.roll(middle, 4, 0), low]).astype(BF16)


def run_tiles(table, target, lt, ra, right, moment, packed_row, acc_a, acc_b, scratch):
    s0, s1, p0, p1 = scratch
    s0[...] = jnp.ones_like(s0)
    p0[...] = jnp.zeros_like(p0)

    def bins(f):
        return jnp.minimum(f >> 7, BINS - 1), f & 127

    def times(f):
        return (table[f >> 7, f & 127] >> 13).astype(F32)

    def distances(tiles, s_ref):
        for n, f in enumerate(tiles):
            a, b = bins(f)
            s_ref[n] = jnp.dot(lt[a], right[b], preferred_element_type=F32)

    def weights(tiles, s_ref, p_ref):
        for n, f in enumerate(tiles):
            a, b = bins(f)
            r_b = packed_row(b)
            for g in range(8):
                rows = slice(16 * g, 16 * g + 16)
                s = s_ref[n, rows, :]
                v = jnp.maximum((ra[a, rows, :] + r_b) * lax.rsqrt(s) - 1.0, TINY)
                square = v * v
                w = square * lax.rsqrt(square + v)
                high = w.astype(BF16)
                low = (w - high.astype(F32)).astype(BF16)
                p_ref[n, 0, rows, :] = high
                p_ref[n, 1, rows, :] = low

    def forces(tiles, p_ref):
        for q in range(0, TILES, 2):
            a1, b1 = bins(tiles[q])
            a2, b2 = bins(tiles[q + 1])
            high1, low1 = p_ref[q, 0], p_ref[q, 1]
            high2, low2 = p_ref[q + 1, 0], p_ref[q + 1, 1]
            scale1, scale2 = times(tiles[q]), times(tiles[q + 1])
            if acc_b is not None:
                c1, c2 = target(a1, b1), target(a2, b2)
                m = jnp.concatenate([moment[a1], moment[a2]], axis=0)
                both = jnp.concatenate(
                    [
                        jnp.concatenate([high1, high2], axis=1),
                        jnp.concatenate([low1, low2], axis=1),
                    ],
                    axis=0,
                )
                out = jnp.dot(
                    jnp.concatenate([m, m], axis=1), both, preferred_element_type=F32
                )
                acc_b[c1] += scale1 * out[:16, :128]
                acc_b[c2] += scale2 * out[16:, 128:]
            m = jnp.concatenate([moment[b1], moment[b2]], axis=0)
            out = lax.dot_general(
                jnp.concatenate([m, m], axis=1),
                jnp.concatenate(
                    [
                        jnp.concatenate([high1, low1], axis=1),
                        jnp.concatenate([high2, low2], axis=1),
                    ],
                    axis=0,
                ),
                (((1,), (1,)), ((), ())),
                preferred_element_type=F32,
            )
            acc_a[a1] += scale1 * out[:16, :128]
            acc_a[a2] += scale2 * out[16:, 128:]

    def following(f):
        return table[f >> 7, f & 127] & (PLACES - 1)

    def draw(f):
        tiles = []
        for _ in range(TILES):
            tiles.append(f)
            f = following(jnp.minimum(f + 1, END))
        return f, tuple(tiles)

    none = (jnp.int32(END),) * TILES

    def body(count, _, carry):
        f, second, third = carry
        for half in range(count):
            f, first = draw(f)
            s_from, s_to, p_from, p_to = (s0, s1, p0, p1) if half % 2 == 0 else (s1, s0, p1, p0)
            forces(third, p_from)
            weights(second, s_from, p_to)
            distances(first, s_to)
            second, third = first, second
        return f, second, third

    live = table[BINS + 1, 0]
    halves = (live + TILES - 1) // TILES + 2
    long = halves // HALVES
    short = (halves - long * HALVES + 1) // 2
    carry = (following(jnp.int32(0)), none, none)
    carry = lax.fori_loop(0, long, functools.partial(body, HALVES), carry)
    lax.fori_loop(0, short, functools.partial(body, 2), carry)


def own_kernel(table_v, packed, acc, lt, ra, new_positions, places, sent, table, loaded, right_b, moment_b, acc_b, *scratch):
    load = pltpu.make_async_copy(table_v, table, loaded)
    load.start()
    for c in range(3):
        places[c] = packed[:BINS, c, :]
    send = pltpu.make_async_copy(places, new_positions, sent)
    send.start()
    depth = lax.broadcasted_iota(jnp.int32, (DEPTH, 128), 0)
    choose = ((depth == 5) | (depth == 21) | (depth == 45)).astype(BF16)

    def turn(n, carry):
        right, left, moment = bin_rows(packed[n])
        right_b[n] = right_operand(right)
        moment_b[n] = moment_operand(moment)
        columns = left_operand(left)
        lt[n] = columns
        ra[n] = jnp.dot(columns, choose, preferred_element_type=F32)
        return carry

    lax.fori_loop(0, BINS, turn, 0, unroll=8)
    acc[...] = jnp.zeros_like(acc)
    acc_b[...] = jnp.zeros_like(acc_b)
    load.wait()
    run_tiles(table, lambda a, b: jnp.where(a == b, BINS, b), lt, ra, right_b, moment_b,
              lambda b: packed[b, pl.ds(3, 1), :], acc, acc_b, scratch)
    acc[...] += acc_b[:BINS]
    send.wait()


def cross_kernel(upward, even, odd, packed, velocity, old_force, acc_in, lt, ra,
                 new_velocity, new_force, right_b, moment_b, radii, acc,
                 table_v, table, loaded, *scratch):
    is_up = upward[0] > 0
    row, lane = iotas(BINS)

    def counts_of(ref):
        return jnp.concatenate([ref[BINS + n] for n in range(BINS // 4)])

    mine = counts_of(packed)
    lower = jnp.where((lane >= BINS - GHOSTS) & (lane < BINS), pltpu.roll(mine, BINS - GHOSTS, 1), 0.0)
    upper = jnp.where(lane < GHOSTS, pltpu.roll(mine, 128 - BINS - GHOSTS, 1), 0.0)
    blank = jnp.zeros((BINS - GHOSTS, 128), F32)

    def with_partner(counts, above):
        flipped = widened(jnp.transpose(counts))
        above_part = upper + jnp.concatenate([blank, flipped[:GHOSTS]])
        below_part = lower + jnp.concatenate([flipped[BINS + GHOSTS : BINS + 2 * GHOSTS], blank])
        return jnp.where(above, above_part, below_part)

    by_even = with_partner(counts_of(even), is_up)
    by_odd = with_partner(counts_of(odd), jnp.logical_not(is_up))
    table_v[...] = table_of(by_even + pltpu.roll(by_odd, BINS, 1), 6)
    load = pltpu.make_async_copy(table_v, table, loaded)
    load.start()

    def turn(n, carry):
        for ref, base in ((even, 0), (odd, BINS)):
            cell = ref[n]
            right, _, moment = bin_rows(cell)
            right_b[base + n] = right_operand(right)
            moment_b[base + n] = moment_operand(moment)
            radii[base + n] = cell[3:4]
        return carry

    lax.fori_loop(0, BINS, turn, 0, unroll=4)
    acc[...] = acc_in[...]
    load.wait()
    run_tiles(table, None, lt, ra, right_b, moment_b, lambda b: radii[b], acc, None, scratch)
    radius = packed[:BINS, 3, :]
    sigma = jnp.sqrt(10.0 * radius)
    scale = 1.0 / (125.0 * radius * radius * radius)

    def gathered(c):
        return acc[:, c, :] + acc[:, 4 + c, :] + acc[:, 8 + c, :]

    total = gathered(3)
    for c in range(3):
        force = sigma * ((packed[:BINS, c, :] - 0.5) * total - gathered(c))
        new_force[c] = force
        gravity = -0.5 if c == 1 else 0.0
        accel = (old_force[c] * scale + gravity) + (force * scale + gravity)
        new_velocity[c] = velocity[c] + 0.5 * TIMESTEP * accel


VMEM = pl.BlockSpec(memory_space=pltpu.VMEM)
SMEM = pl.BlockSpec(memory_space=pltpu.SMEM)
HBM = pl.BlockSpec(memory_space=pltpu.HBM)


def pipeline_scratch():
    return [
        pltpu.VMEM((TILES, 128, 128), F32),
        pltpu.VMEM((TILES, 128, 128), F32),
        pltpu.VMEM((TILES, 2, 128, 128), BF16),
        pltpu.VMEM((TILES, 2, 128, 128), BF16),
    ]


def local(positions, radius, velocity, old_force, neighbours, tile_count):
    def by_component(cells):
        return jnp.transpose(cells, (1, 0, 2))

    positions, velocity, old_force = map(by_component, (positions, velocity, old_force))
    cells = jax.ShapeDtypeStruct((3, BINS, 128), F32)
    slots = neighbours.shape[1]
    component = lax.broadcasted_iota(jnp.int32, (5, BINS, 128), 0)
    five = ((0, 2), (0, 0), (0, 0))
    each_radius = jnp.where(component < 3, radius[None], 1.0)
    accel = jnp.pad(old_force, five) / (125.0 * each_radius * each_radius * each_radius)
    accel = accel + jnp.where(component == 1, -0.5, 0.0)
    moved = jnp.pad(positions, five) + TIMESTEP * jnp.pad(velocity, five) + 0.5 * TIMESTEP * TIMESTEP * accel
    planes = jnp.where(component < 3, moved, radius[None])
    listed = jnp.pad(neighbours.T[None], ((4, 0), (0, BINS - slots), (0, 128 - BINS)))
    counted = jnp.pad(tile_count[None, None], ((4, 0), (BINS - 1, 0), (0, 128 - BINS)))
    planes = jnp.where(component < 4, planes, (listed + counted).astype(F32))
    packed, own_table = pl.pallas_call(
        functools.partial(prologue_kernel, slots),
        out_shape=(
            jax.ShapeDtypeStruct((BINS + 8, 4, 128), F32),
            jax.ShapeDtypeStruct((BINS + 8, 128), jnp.int32),
        ),
        in_specs=[VMEM],
        out_specs=(VMEM,) * 2,
        compiler_params=pltpu.CompilerParams(vmem_limit_bytes=8 << 20),
        name="prologue",
    )(planes)

    slabs = lax.axis_size("slab")
    swap_even = [(i + d, i + 1 - d) for i in range(0, slabs - 1, 2) for d in (0, 1)]
    swap_odd = [(i + d, i + 1 - d) for i in range(1, slabs - 1, 2) for d in (0, 1)]
    even = lax.ppermute(packed, "slab", swap_even)
    odd = lax.ppermute(packed, "slab", swap_odd)

    acc, lt, ra, new_positions = pl.pallas_call(
        own_kernel,
        out_shape=(
            jax.ShapeDtypeStruct((BINS, 16, 128), F32),
            jax.ShapeDtypeStruct((BINS, 128, DEPTH), BF16),
            jax.ShapeDtypeStruct((BINS, 128, 128), F32),
            cells,
        ),
        in_specs=[VMEM, VMEM],
        out_specs=(VMEM, VMEM, VMEM, HBM),
        scratch_shapes=[
            pltpu.VMEM((3, BINS, 128), F32),
            pltpu.SemaphoreType.DMA,
            pltpu.SMEM((BINS + 8, 128), jnp.int32),
            pltpu.SemaphoreType.DMA,
            pltpu.VMEM((BINS, DEPTH, 128), BF16),
            pltpu.VMEM((BINS, 16, 128), BF16),
            pltpu.VMEM((BINS + 1, 16, 128), F32),
            *pipeline_scratch(),
        ],
        compiler_params=pltpu.CompilerParams(vmem_limit_bytes=16 << 20),
        cost_estimate=pl.CostEstimate(flops=10**9, bytes_accessed=10**6, transcendentals=0),
        name="own_tiles",
    )(own_table, packed)

    upward = (1 - lax.axis_index("slab") % 2).astype(jnp.int32)[None]
    new_velocity, new_force = pl.pallas_call(
        cross_kernel,
        out_shape=(cells, cells),
        in_specs=[SMEM] + [VMEM] * 8,
        out_specs=(VMEM, VMEM),
        scratch_shapes=[
            pltpu.VMEM((2 * BINS, DEPTH, 128), BF16),
            pltpu.VMEM((2 * BINS, 16, 128), BF16),
            pltpu.VMEM((2 * BINS, 1, 128), F32),
            pltpu.VMEM((BINS, 16, 128), F32),
            pltpu.VMEM((BINS + 8, 128), jnp.int32),
            pltpu.SMEM((BINS + 8, 128), jnp.int32),
            pltpu.SemaphoreType.DMA,
            *pipeline_scratch(),
        ],
        compiler_params=pltpu.CompilerParams(vmem_limit_bytes=16 << 20),
        cost_estimate=pl.CostEstimate(flops=10**9, bytes_accessed=10**6, transcendentals=0),
        name="cross_tiles",
    )(upward, even, odd, packed, velocity, old_force, acc, lt, ra)
    return tuple(map(by_component, (new_positions, new_velocity, new_force)))


def solution(mesh):
    flat = P(("slab", "blk"))
    rows = P(("slab", "blk"), None)
    cells = P(("slab", "blk"), None, None)
    return jax.shard_map(
        local,
        mesh=mesh,
        in_specs=(cells, rows, cells, cells, rows, flat),
        out_specs=(cells, cells, cells),
        check_vma=False,
    )
```

```python
import functools

import jax
import jax.numpy as jnp
from jax import lax
from jax.experimental import pallas as pl
from jax.experimental.pallas import tpu as pltpu
from jax.sharding import PartitionSpec as P

GHOSTS = 8
TIMESTEP = 0.2
TINY = 1e-25
TILES = 4
BINS = 32
DEPTH = 48
END = BINS * 128
PLACES = 8192
HALVES = 8
F32 = jnp.float32
BF16 = jnp.bfloat16


def rounded(value):
    return value.astype(BF16).astype(F32)


def split3(value):
    high = rounded(value)
    middle = rounded(value - high)
    return high, middle, value - high - middle


def iotas(rows):
    shape = (rows, 128)
    return lax.broadcasted_iota(jnp.int32, shape, 0), lax.broadcasted_iota(jnp.int32, shape, 1)


def widened(value):
    rows, lanes = value.shape
    return jnp.concatenate([value, jnp.zeros((rows, 128 - lanes), value.dtype)], axis=1)


def table_of(weight, span):
    row, lane = iotas(BINS)
    step = jnp.where(weight > 0.0, row * 128 + lane, END)
    for s in (1, 2, 4, 8, 16, 32)[:span]:
        ahead = pltpu.roll(step, 128 - s, 1)
        step = jnp.minimum(step, jnp.where(lane + s < 128, ahead, END))
    later = jnp.broadcast_to(step[:, :1], (BINS, 128))
    later = jnp.where(row + 1 < BINS, pltpu.roll(later, BINS - 1, 0), END)
    for s in (1, 2, 4, 8, 16):
        ahead = pltpu.roll(later, BINS - s, 0)
        later = jnp.minimum(later, jnp.where(row + s < BINS, ahead, END))
    live = jnp.sum(jnp.where(weight > 0.0, 1.0, 0.0), axis=1, keepdims=True)
    live = jnp.broadcast_to(jnp.sum(live, axis=0, keepdims=True), (8, 128)).astype(jnp.int32)
    tail, _ = iotas(8)
    tail = jnp.where(tail == 1, live, END)
    return jnp.concatenate([jnp.minimum(step, later) + PLACES * weight.astype(jnp.int32), tail])


def prologue_kernel(slots, planes, packed, table):
    for c in range(4):
        packed[:BINS, c, :] = planes[c]
    slot = lax.broadcasted_iota(jnp.int32, (slots, 128), 0).astype(F32)
    marked = jnp.where(slot < planes[4, pl.ds(BINS - 1, 1), :], planes[4, :slots, :], -1.0)
    marked = jnp.transpose(marked)[:BINS]
    row, lane = iotas(BINS)
    candidate = lane.astype(F32)
    counts = jnp.zeros((BINS, 128), F32)
    for k in range(slots):
        counts = counts + jnp.where(marked[:, k : k + 1] == candidate, 1.0, 0.0)
    for n in range(BINS // 4):
        packed[BINS + n] = counts[4 * n : 4 * n + 4]
    inner = jnp.where(lane < BINS, pltpu.roll(counts, 128 - GHOSTS, 1), 0.0)
    mirror = widened(jnp.transpose(inner)[:BINS])
    pairs = jnp.where(lane > row, inner + mirror, 0.0)
    table[...] = table_of(jnp.where(lane == row, 1.0, pairs), 5)


def bin_rows(cell):
    cell = jnp.concatenate([cell, jnp.zeros((4, 128), F32)])
    row = lax.broadcasted_iota(jnp.int32, (8, 128), 0)
    radius = cell[3:4]
    sigma = jnp.sqrt(10.0 * radius)
    place = jnp.where(row < 3, cell - 0.5, 0.0)
    square = place * place
    norm = square[0:1] + square[1:2] + square[2:3]
    right = jnp.where(row == 3, 1.0, jnp.where(row == 4, norm + 0.0025, -2.0 * place))
    left = jnp.where(row == 3, norm, jnp.where(row == 4, 1.0, jnp.where(row == 5, radius, place)))
    moment = sigma * jnp.where(row == 3, 1.0, place)
    return right, left, moment


def right_operand(rows):
    high, middle, low = split3(rows)
    return jnp.concatenate([high, middle, high, middle, low, high]).astype(BF16)


def left_operand(rows):
    high, middle, low = split3(rows)
    return jnp.transpose(jnp.concatenate([high, high, middle, middle, high, low])).astype(BF16)


def moment_operand(rows):
    high, middle, low = split3(rows)
    return jnp.concatenate([high + pltpu.roll(middle, 4, 0), low]).astype(BF16)


def run_tiles(table, target, lt, ra, right, moment, packed_row, acc_a, acc_b, scratch):
    s0, s1, p0, p1 = scratch
    s0[...] = jnp.ones_like(s0)
    p0[...] = jnp.zeros_like(p0)

    def bins(f):
        return jnp.minimum(f >> 7, BINS - 1), f & 127

    def times(f):
        return (table[f >> 7, f & 127] >> 13).astype(F32)

    def distances(tiles, s_ref):
        for n, f in enumerate(tiles):
            a, b = bins(f)
            s_ref[n] = jnp.dot(lt[a], right[b], preferred_element_type=F32)

    def weights(tiles, s_ref, p_ref):
        for n, f in enumerate(tiles):
            a, b = bins(f)
            r_b = packed_row(b)
            for g in range(8):
                rows = slice(16 * g, 16 * g + 16)
                s = s_ref[n, rows, :]
                v = jnp.maximum((ra[a, rows, :] + r_b) * lax.rsqrt(s) - 1.0, TINY)
                square = v * v
                w = square * lax.rsqrt(square + v)
                high = w.astype(BF16)
                low = (w - high.astype(F32)).astype(BF16)
                p_ref[n, 0, rows, :] = high
                p_ref[n, 1, rows, :] = low

    def forces(tiles, p_ref):
        for q in range(0, TILES, 2):
            a1, b1 = bins(tiles[q])
            a2, b2 = bins(tiles[q + 1])
            high1, low1 = p_ref[q, 0], p_ref[q, 1]
            high2, low2 = p_ref[q + 1, 0], p_ref[q + 1, 1]
            scale1, scale2 = times(tiles[q]), times(tiles[q + 1])
            if acc_b is not None:
                c1, c2 = target(a1, b1), target(a2, b2)
                m = jnp.concatenate([moment[a1], moment[a2]], axis=0)
                both = jnp.concatenate(
                    [
                        jnp.concatenate([high1, high2], axis=1),
                        jnp.concatenate([low1, low2], axis=1),
                    ],
                    axis=0,
                )
                out = jnp.dot(
                    jnp.concatenate([m, m], axis=1), both, preferred_element_type=F32
                )
                acc_b[c1] += scale1 * out[:16, :128]
                acc_b[c2] += scale2 * out[16:, 128:]
            m = jnp.concatenate([moment[b1], moment[b2]], axis=0)
            out = lax.dot_general(
                jnp.concatenate([m, m], axis=1),
                jnp.concatenate(
                    [
                        jnp.concatenate([high1, low1], axis=1),
                        jnp.concatenate([high2, low2], axis=1),
                    ],
                    axis=0,
                ),
                (((1,), (1,)), ((), ())),
                preferred_element_type=F32,
            )
            acc_a[a1] += scale1 * out[:16, :128]
            acc_a[a2] += scale2 * out[16:, 128:]

    def following(f):
        return table[f >> 7, f & 127] & (PLACES - 1)

    def draw(f):
        tiles = []
        for _ in range(TILES):
            tiles.append(f)
            f = following(jnp.minimum(f + 1, END))
        return f, tuple(tiles)

    none = (jnp.int32(END),) * TILES

    def body(count, _, carry):
        f, second, third = carry
        for half in range(count):
            f, first = draw(f)
            s_from, s_to, p_from, p_to = (s0, s1, p0, p1) if half % 2 == 0 else (s1, s0, p1, p0)
            forces(third, p_from)
            weights(second, s_from, p_to)
            distances(first, s_to)
            second, third = first, second
        return f, second, third

    live = table[BINS + 1, 0]
    halves = (live + TILES - 1) // TILES + 2
    long = halves // HALVES
    short = (halves - long * HALVES + 1) // 2
    carry = (following(jnp.int32(0)), none, none)
    carry = lax.fori_loop(0, long, functools.partial(body, HALVES), carry)
    lax.fori_loop(0, short, functools.partial(body, 2), carry)


def own_kernel(table_v, packed, acc, lt, ra, new_positions, places, sent, table, loaded, right_b, moment_b, acc_b, *scratch):
    load = pltpu.make_async_copy(table_v, table, loaded)
    load.start()
    for c in range(3):
        places[c] = packed[:BINS, c, :]
    send = pltpu.make_async_copy(places, new_positions, sent)
    send.start()
    depth = lax.broadcasted_iota(jnp.int32, (DEPTH, 128), 0)
    choose = ((depth == 5) | (depth == 21) | (depth == 45)).astype(BF16)

    def turn(n, carry):
        right, left, moment = bin_rows(packed[n])
        right_b[n] = right_operand(right)
        moment_b[n] = moment_operand(moment)
        columns = left_operand(left)
        lt[n] = columns
        ra[n] = jnp.dot(columns, choose, preferred_element_type=F32)
        return carry

    lax.fori_loop(0, BINS, turn, 0, unroll=32)
    acc[...] = jnp.zeros_like(acc)
    acc_b[...] = jnp.zeros_like(acc_b)
    load.wait()
    run_tiles(table, lambda a, b: jnp.where(a == b, BINS, b), lt, ra, right_b, moment_b,
              lambda b: packed[b, pl.ds(3, 1), :], acc, acc_b, scratch)
    acc[...] += acc_b[:BINS]
    send.wait()


def cross_kernel(upward, odd, even, packed, velocity, old_force, acc_in, lt, ra,
                 new_velocity, new_force, right_b, moment_b, radii, acc,
                 table_v, table, loaded, *scratch):
    is_up = upward[0] > 0
    row, lane = iotas(BINS)

    def counts_of(ref):
        return jnp.concatenate([ref[BINS + n] for n in range(BINS // 4)])

    mine = counts_of(packed)
    lower = jnp.where((lane >= BINS - GHOSTS) & (lane < BINS), pltpu.roll(mine, BINS - GHOSTS, 1), 0.0)
    upper = jnp.where(lane < GHOSTS, pltpu.roll(mine, 128 - BINS - GHOSTS, 1), 0.0)
    blank = jnp.zeros((BINS - GHOSTS, 128), F32)

    def with_partner(counts, above):
        flipped = widened(jnp.transpose(counts))
        above_part = upper + jnp.concatenate([blank, flipped[:GHOSTS]])
        below_part = lower + jnp.concatenate([flipped[BINS + GHOSTS : BINS + 2 * GHOSTS], blank])
        return jnp.where(above, above_part, below_part)

    by_even = with_partner(counts_of(even), is_up)
    by_odd = with_partner(counts_of(odd), jnp.logical_not(is_up))
    table_v[...] = table_of(by_even + pltpu.roll(by_odd, BINS, 1), 6)
    load = pltpu.make_async_copy(table_v, table, loaded)
    load.start()

    def turn(n, carry):
        for ref, base in ((even, 0), (odd, BINS)):
            cell = ref[n]
            right, _, moment = bin_rows(cell)
            right_b[base + n] = right_operand(right)
            moment_b[base + n] = moment_operand(moment)
            radii[base + n] = cell[3:4]
        return carry

    lax.fori_loop(0, BINS, turn, 0, unroll=16)
    acc[...] = acc_in[...]
    load.wait()
    run_tiles(table, None, lt, ra, right_b, moment_b, lambda b: radii[b], acc, None, scratch)
    for n in range(BINS):
        cell = packed[n]
        sums = acc[n]
        sums = sums[0:4] + sums[4:8] + sums[8:12]
        force = jnp.sqrt(10.0 * cell[3:4]) * ((cell - 0.5) * sums[3:4] - sums)
        for c in range(3):
            new_force[c, pl.ds(n, 1), :] = force[c : c + 1]
    radius = packed[:BINS, 3, :]
    scale = 1.0 / (125.0 * radius * radius * radius)
    for c in range(3):
        gravity = -0.5 if c == 1 else 0.0
        accel = (old_force[c] * scale + gravity) + (new_force[c] * scale + gravity)
        new_velocity[c] = velocity[c] + 0.5 * TIMESTEP * accel


VMEM = pl.BlockSpec(memory_space=pltpu.VMEM)
SMEM = pl.BlockSpec(memory_space=pltpu.SMEM)
HBM = pl.BlockSpec(memory_space=pltpu.HBM)


def pipeline_scratch():
    return [
        pltpu.VMEM((TILES, 128, 128), F32),
        pltpu.VMEM((TILES, 128, 128), F32),
        pltpu.VMEM((TILES, 2, 128, 128), BF16),
        pltpu.VMEM((TILES, 2, 128, 128), BF16),
    ]


def local(positions, radius, velocity, old_force, neighbours, tile_count):
    def by_component(cells):
        return jnp.transpose(cells, (1, 0, 2))

    positions, velocity, old_force = map(by_component, (positions, velocity, old_force))
    cells = jax.ShapeDtypeStruct((3, BINS, 128), F32)
    slots = neighbours.shape[1]
    component = lax.broadcasted_iota(jnp.int32, (5, BINS, 128), 0)
    five = ((0, 2), (0, 0), (0, 0))
    each_radius = jnp.where(component < 3, radius[None], 1.0)
    accel = jnp.pad(old_force, five) / (125.0 * each_radius * each_radius * each_radius)
    accel = accel + jnp.where(component == 1, -0.5, 0.0)
    moved = jnp.pad(positions, five) + TIMESTEP * jnp.pad(velocity, five) + 0.5 * TIMESTEP * TIMESTEP * accel
    planes = jnp.where(component < 3, moved, radius[None])
    listed = jnp.pad(neighbours.T[None], ((4, 0), (0, BINS - slots), (0, 128 - BINS)))
    counted = jnp.pad(tile_count[None, None], ((4, 0), (BINS - 1, 0), (0, 128 - BINS)))
    planes = jnp.where(component < 4, planes, (listed + counted).astype(F32))
    packed, own_table = pl.pallas_call(
        functools.partial(prologue_kernel, slots),
        out_shape=(
            jax.ShapeDtypeStruct((BINS + 8, 4, 128), F32),
            jax.ShapeDtypeStruct((BINS + 8, 128), jnp.int32),
        ),
        in_specs=[VMEM],
        out_specs=(VMEM,) * 2,
        compiler_params=pltpu.CompilerParams(vmem_limit_bytes=8 << 20),
        name="prologue",
    )(planes)

    slabs = lax.axis_size("slab")
    swap_even = [(i + d, i + 1 - d) for i in range(0, slabs - 1, 2) for d in (0, 1)]
    swap_odd = [(i + d, i + 1 - d) for i in range(1, slabs - 1, 2) for d in (0, 1)]
    even = lax.ppermute(packed, "slab", swap_even)
    odd = lax.ppermute(packed, "slab", swap_odd)

    acc, lt, ra, new_positions = pl.pallas_call(
        own_kernel,
        out_shape=(
            jax.ShapeDtypeStruct((BINS, 16, 128), F32),
            jax.ShapeDtypeStruct((BINS, 128, DEPTH), BF16),
            jax.ShapeDtypeStruct((BINS, 128, 128), F32),
            cells,
        ),
        in_specs=[VMEM, VMEM],
        out_specs=(VMEM, VMEM, VMEM, HBM),
        scratch_shapes=[
            pltpu.VMEM((3, BINS, 128), F32),
            pltpu.SemaphoreType.DMA,
            pltpu.SMEM((BINS + 8, 128), jnp.int32),
            pltpu.SemaphoreType.DMA,
            pltpu.VMEM((BINS, DEPTH, 128), BF16),
            pltpu.VMEM((BINS, 16, 128), BF16),
            pltpu.VMEM((BINS + 1, 16, 128), F32),
            *pipeline_scratch(),
        ],
        compiler_params=pltpu.CompilerParams(vmem_limit_bytes=16 << 20),
        cost_estimate=pl.CostEstimate(flops=10**9, bytes_accessed=10**6, transcendentals=0),
        name="own_tiles",
    )(own_table, packed)

    upward = (1 - lax.axis_index("slab") % 2).astype(jnp.int32)[None]
    new_velocity, new_force = pl.pallas_call(
        cross_kernel,
        out_shape=(cells, cells),
        in_specs=[SMEM] + [VMEM] * 8,
        out_specs=(VMEM, VMEM),
        scratch_shapes=[
            pltpu.VMEM((2 * BINS, DEPTH, 128), BF16),
            pltpu.VMEM((2 * BINS, 16, 128), BF16),
            pltpu.VMEM((2 * BINS, 1, 128), F32),
            pltpu.VMEM((BINS, 16, 128), F32),
            pltpu.VMEM((BINS + 8, 128), jnp.int32),
            pltpu.SMEM((BINS + 8, 128), jnp.int32),
            pltpu.SemaphoreType.DMA,
            *pipeline_scratch(),
        ],
        compiler_params=pltpu.CompilerParams(vmem_limit_bytes=16 << 20),
        cost_estimate=pl.CostEstimate(flops=10**9, bytes_accessed=10**6, transcendentals=0),
        name="cross_tiles",
    )(upward, odd, even, packed, velocity, old_force, acc, lt, ra)
    return tuple(map(by_component, (new_positions, new_velocity, new_force)))


def solution(mesh):
    flat = P(("slab", "blk"))
    rows = P(("slab", "blk"), None)
    cells = P(("slab", "blk"), None, None)
    return jax.shard_map(
        local,
        mesh=mesh,
        in_specs=(cells, rows, cells, cells, rows, flat),
        out_specs=(cells, cells, cells),
        check_vma=False,
    )
```

```python
import functools

import jax
import jax.numpy as jnp
from jax import lax
from jax.experimental import pallas as pl
from jax.experimental.pallas import tpu as pltpu
from jax.sharding import PartitionSpec as P

GHOSTS = 8
TIMESTEP = 0.2
TINY = 1e-25
TILES = 4
BINS = 32
DEPTH = 48
END = BINS * 128
PLACES = 8192
TRIPS = (16, 8, 2)
F32 = jnp.float32
BF16 = jnp.bfloat16


def rounded(value):
    return value.astype(BF16).astype(F32)


def split3(value):
    high = rounded(value)
    middle = rounded(value - high)
    return high, middle, value - high - middle


def iotas(rows):
    shape = (rows, 128)
    return lax.broadcasted_iota(jnp.int32, shape, 0), lax.broadcasted_iota(jnp.int32, shape, 1)


def widened(value):
    rows, lanes = value.shape
    return jnp.concatenate([value, jnp.zeros((rows, 128 - lanes), value.dtype)], axis=1)


def table_of(weight, span):
    row, lane = iotas(BINS)
    step = jnp.where(weight > 0.0, row * 128 + lane, END)
    for s in (1, 2, 4, 8, 16, 32)[:span]:
        ahead = pltpu.roll(step, 128 - s, 1)
        step = jnp.minimum(step, jnp.where(lane + s < 128, ahead, END))
    later = jnp.broadcast_to(step[:, :1], (BINS, 128))
    later = jnp.where(row + 1 < BINS, pltpu.roll(later, BINS - 1, 0), END)
    for s in (1, 2, 4, 8, 16):
        ahead = pltpu.roll(later, BINS - s, 0)
        later = jnp.minimum(later, jnp.where(row + s < BINS, ahead, END))
    live = jnp.sum(jnp.where(weight > 0.0, 1.0, 0.0), axis=1, keepdims=True)
    live = jnp.broadcast_to(jnp.sum(live, axis=0, keepdims=True), (8, 128)).astype(jnp.int32)
    tail, _ = iotas(8)
    tail = jnp.where(tail == 1, live, END)
    return jnp.concatenate([jnp.minimum(step, later) + PLACES * weight.astype(jnp.int32), tail])


def prologue_kernel(slots, planes, packed, table):
    for c in range(4):
        packed[:BINS, c, :] = planes[c]
    slot = lax.broadcasted_iota(jnp.int32, (slots, 128), 0).astype(F32)
    marked = jnp.where(slot < planes[4, pl.ds(BINS - 1, 1), :], planes[4, :slots, :], -1.0)
    marked = jnp.transpose(marked)[:BINS]
    row, lane = iotas(BINS)
    candidate = lane.astype(F32)
    counts = jnp.zeros((BINS, 128), F32)
    for k in range(slots):
        counts = counts + jnp.where(marked[:, k : k + 1] == candidate, 1.0, 0.0)
    for n in range(BINS // 4):
        packed[BINS + n] = counts[4 * n : 4 * n + 4]
    inner = jnp.where(lane < BINS, pltpu.roll(counts, 128 - GHOSTS, 1), 0.0)
    mirror = widened(jnp.transpose(inner)[:BINS])
    pairs = jnp.where(lane > row, inner + mirror, 0.0)
    table[...] = table_of(jnp.where(lane == row, 1.0, pairs), 5)


def bin_rows(cell):
    cell = jnp.concatenate([cell, jnp.zeros((4, 128), F32)])
    row = lax.broadcasted_iota(jnp.int32, (8, 128), 0)
    radius = cell[3:4]
    sigma = jnp.sqrt(10.0 * radius)
    place = jnp.where(row < 3, cell - 0.5, 0.0)
    square = place * place
    norm = square[0:1] + square[1:2] + square[2:3]
    right = jnp.where(row == 3, 1.0, jnp.where(row == 4, norm + 0.0025, -2.0 * place))
    left = jnp.where(row == 3, norm, jnp.where(row == 4, 1.0, jnp.where(row == 5, radius, place)))
    moment = sigma * jnp.where(row == 3, 1.0, place)
    return right, left, moment


def right_operand(rows):
    high, middle, low = split3(rows)
    return jnp.concatenate([high, middle, high, middle, low, high]).astype(BF16)


def left_operand(rows):
    high, middle, low = split3(rows)
    return jnp.transpose(jnp.concatenate([high, high, middle, middle, high, low])).astype(BF16)


def moment_operand(rows):
    high, middle, low = split3(rows)
    return jnp.concatenate([high + pltpu.roll(middle, 4, 0), low]).astype(BF16)


def run_tiles(table, target, lt, ra, right, moment, packed_row, acc_a, acc_b, scratch):
    s0, s1, p0, p1 = scratch
    s0[...] = jnp.ones_like(s0)
    p0[...] = jnp.zeros_like(p0)

    def bins(f):
        return jnp.minimum(f >> 7, BINS - 1), f & 127

    def times(f):
        return (table[f >> 7, f & 127] >> 13).astype(F32)

    def distances(tiles, s_ref):
        for n, f in enumerate(tiles):
            a, b = bins(f)
            s_ref[n] = jnp.dot(lt[a], right[b], preferred_element_type=F32)

    def weights(tiles, s_ref, p_ref):
        for n, f in enumerate(tiles):
            a, b = bins(f)
            r_b = packed_row(b)
            for g in range(8):
                rows = slice(16 * g, 16 * g + 16)
                s = s_ref[n, rows, :]
                v = jnp.maximum((ra[a, rows, :] + r_b) * lax.rsqrt(s) - 1.0, TINY)
                square = v * v
                w = square * lax.rsqrt(square + v)
                high = w.astype(BF16)
                low = (w - high.astype(F32)).astype(BF16)
                p_ref[n, 0, rows, :] = high
                p_ref[n, 1, rows, :] = low

    def forces(tiles, p_ref):
        for q in range(0, TILES, 2):
            a1, b1 = bins(tiles[q])
            a2, b2 = bins(tiles[q + 1])
            high1, low1 = p_ref[q, 0], p_ref[q, 1]
            high2, low2 = p_ref[q + 1, 0], p_ref[q + 1, 1]
            scale1, scale2 = times(tiles[q]), times(tiles[q + 1])
            if acc_b is not None:
                c1, c2 = target(a1, b1), target(a2, b2)
                m = jnp.concatenate([moment[a1], moment[a2]], axis=0)
                both = jnp.concatenate(
                    [
                        jnp.concatenate([high1, high2], axis=1),
                        jnp.concatenate([low1, low2], axis=1),
                    ],
                    axis=0,
                )
                out = jnp.dot(
                    jnp.concatenate([m, m], axis=1), both, preferred_element_type=F32
                )
                acc_b[c1] += scale1 * out[:16, :128]
                acc_b[c2] += scale2 * out[16:, 128:]
            m = jnp.concatenate([moment[b1], moment[b2]], axis=0)
            out = lax.dot_general(
                jnp.concatenate([m, m], axis=1),
                jnp.concatenate(
                    [
                        jnp.concatenate([high1, low1], axis=1),
                        jnp.concatenate([high2, low2], axis=1),
                    ],
                    axis=0,
                ),
                (((1,), (1,)), ((), ())),
                preferred_element_type=F32,
            )
            acc_a[a1] += scale1 * out[:16, :128]
            acc_a[a2] += scale2 * out[16:, 128:]

    def following(f):
        return table[f >> 7, f & 127] & (PLACES - 1)

    def draw(f):
        tiles = []
        for _ in range(TILES):
            tiles.append(f)
            f = following(jnp.minimum(f + 1, END))
        return f, tuple(tiles)

    none = (jnp.int32(END),) * TILES

    def body(count, _, carry):
        f, second, third = carry
        for half in range(count):
            f, first = draw(f)
            s_from, s_to, p_from, p_to = (s0, s1, p0, p1) if half % 2 == 0 else (s1, s0, p1, p0)
            forces(third, p_from)
            weights(second, s_from, p_to)
            distances(first, s_to)
            second, third = first, second
        return f, second, third

    live = table[BINS + 1, 0]
    halves = (live + TILES - 1) // TILES + 2
    carry = (following(jnp.int32(0)), none, none)
    for count in TRIPS:
        last = count == TRIPS[-1]
        trips = (halves + count - 1) // count if last else halves // count
        carry = lax.fori_loop(0, trips, functools.partial(body, count), carry)
        halves = halves - trips * count


def own_kernel(table_v, packed, acc, lt, ra, new_positions, places, sent, table, loaded, right_b, moment_b, acc_b, *scratch):
    load = pltpu.make_async_copy(table_v, table, loaded)
    load.start()
    for c in range(3):
        places[c] = packed[:BINS, c, :]
    send = pltpu.make_async_copy(places, new_positions, sent)
    send.start()
    depth = lax.broadcasted_iota(jnp.int32, (DEPTH, 128), 0)
    choose = ((depth == 5) | (depth == 21) | (depth == 45)).astype(BF16)

    def turn(n, carry):
        right, left, moment = bin_rows(packed[n])
        right_b[n] = right_operand(right)
        moment_b[n] = moment_operand(moment)
        columns = left_operand(left)
        lt[n] = columns
        ra[n] = jnp.dot(columns, choose, preferred_element_type=F32)
        return carry

    lax.fori_loop(0, BINS, turn, 0, unroll=32)
    acc[...] = jnp.zeros_like(acc)
    acc_b[...] = jnp.zeros_like(acc_b)
    load.wait()
    run_tiles(table, lambda a, b: jnp.where(a == b, BINS, b), lt, ra, right_b, moment_b,
              lambda b: packed[b, pl.ds(3, 1), :], acc, acc_b, scratch)
    acc[...] += acc_b[:BINS]
    send.wait()


def cross_kernel(upward, odd, even, packed, velocity, old_force, acc_in, lt, ra,
                 new_velocity, new_force, right_b, moment_b, radii, acc,
                 table_v, table, loaded, *scratch):
    is_up = upward[0] > 0
    row, lane = iotas(BINS)

    def counts_of(ref):
        return jnp.concatenate([ref[BINS + n] for n in range(BINS // 4)])

    mine = counts_of(packed)
    lower = jnp.where((lane >= BINS - GHOSTS) & (lane < BINS), pltpu.roll(mine, BINS - GHOSTS, 1), 0.0)
    upper = jnp.where(lane < GHOSTS, pltpu.roll(mine, 128 - BINS - GHOSTS, 1), 0.0)
    blank = jnp.zeros((BINS - GHOSTS, 128), F32)

    def with_partner(counts, above):
        flipped = widened(jnp.transpose(counts))
        above_part = upper + jnp.concatenate([blank, flipped[:GHOSTS]])
        below_part = lower + jnp.concatenate([flipped[BINS + GHOSTS : BINS + 2 * GHOSTS], blank])
        return jnp.where(above, above_part, below_part)

    by_even = with_partner(counts_of(even), is_up)
    by_odd = with_partner(counts_of(odd), jnp.logical_not(is_up))
    table_v[...] = table_of(by_even + pltpu.roll(by_odd, BINS, 1), 6)
    load = pltpu.make_async_copy(table_v, table, loaded)
    load.start()

    def turn(n, carry):
        for ref, base in ((even, 0), (odd, BINS)):
            cell = ref[n]
            right, _, moment = bin_rows(cell)
            right_b[base + n] = right_operand(right)
            moment_b[base + n] = moment_operand(moment)
            radii[base + n] = cell[3:4]
        return carry

    lax.fori_loop(0, BINS, turn, 0, unroll=16)
    acc[...] = acc_in[...]
    load.wait()
    run_tiles(table, None, lt, ra, right_b, moment_b, lambda b: radii[b], acc, None, scratch)
    for n in range(BINS):
        cell = packed[n]
        sums = acc[n]
        sums = sums[0:4] + sums[4:8] + sums[8:12]
        force = jnp.sqrt(10.0 * cell[3:4]) * ((cell - 0.5) * sums[3:4] - sums)
        for c in range(3):
            new_force[c, pl.ds(n, 1), :] = force[c : c + 1]
    radius = packed[:BINS, 3, :]
    scale = 1.0 / (125.0 * radius * radius * radius)
    for c in range(3):
        gravity = -0.5 if c == 1 else 0.0
        accel = (old_force[c] * scale + gravity) + (new_force[c] * scale + gravity)
        new_velocity[c] = velocity[c] + 0.5 * TIMESTEP * accel


VMEM = pl.BlockSpec(memory_space=pltpu.VMEM)
SMEM = pl.BlockSpec(memory_space=pltpu.SMEM)
HBM = pl.BlockSpec(memory_space=pltpu.HBM)


def pipeline_scratch():
    return [
        pltpu.VMEM((TILES, 128, 128), F32),
        pltpu.VMEM((TILES, 128, 128), F32),
        pltpu.VMEM((TILES, 2, 128, 128), BF16),
        pltpu.VMEM((TILES, 2, 128, 128), BF16),
    ]


def local(positions, radius, velocity, old_force, neighbours, tile_count):
    def by_component(cells):
        return jnp.transpose(cells, (1, 0, 2))

    positions, velocity, old_force = map(by_component, (positions, velocity, old_force))
    cells = jax.ShapeDtypeStruct((3, BINS, 128), F32)
    slots = neighbours.shape[1]
    component = lax.broadcasted_iota(jnp.int32, (5, BINS, 128), 0)
    five = ((0, 2), (0, 0), (0, 0))
    each_radius = jnp.where(component < 3, radius[None], 1.0)
    accel = jnp.pad(old_force, five) / (125.0 * each_radius * each_radius * each_radius)
    accel = accel + jnp.where(component == 1, -0.5, 0.0)
    moved = jnp.pad(positions, five) + TIMESTEP * jnp.pad(velocity, five) + 0.5 * TIMESTEP * TIMESTEP * accel
    planes = jnp.where(component < 3, moved, radius[None])
    listed = jnp.pad(neighbours.T[None], ((4, 0), (0, BINS - slots), (0, 128 - BINS)))
    counted = jnp.pad(tile_count[None, None], ((4, 0), (BINS - 1, 0), (0, 128 - BINS)))
    planes = jnp.where(component < 4, planes, (listed + counted).astype(F32))
    packed, own_table = pl.pallas_call(
        functools.partial(prologue_kernel, slots),
        out_shape=(
            jax.ShapeDtypeStruct((BINS + 8, 4, 128), F32),
            jax.ShapeDtypeStruct((BINS + 8, 128), jnp.int32),
        ),
        in_specs=[VMEM],
        out_specs=(VMEM,) * 2,
        compiler_params=pltpu.CompilerParams(vmem_limit_bytes=8 << 20),
        name="prologue",
    )(planes)

    slabs = lax.axis_size("slab")
    swap_even = [(i + d, i + 1 - d) for i in range(0, slabs - 1, 2) for d in (0, 1)]
    swap_odd = [(i + d, i + 1 - d) for i in range(1, slabs - 1, 2) for d in (0, 1)]
    even = lax.ppermute(packed, "slab", swap_even)
    odd = lax.ppermute(packed, "slab", swap_odd)

    acc, lt, ra, new_positions = pl.pallas_call(
        own_kernel,
        out_shape=(
            jax.ShapeDtypeStruct((BINS, 16, 128), F32),
            jax.ShapeDtypeStruct((BINS, 128, DEPTH), BF16),
            jax.ShapeDtypeStruct((BINS, 128, 128), F32),
            cells,
        ),
        in_specs=[VMEM, VMEM],
        out_specs=(VMEM, VMEM, VMEM, HBM),
        scratch_shapes=[
            pltpu.VMEM((3, BINS, 128), F32),
            pltpu.SemaphoreType.DMA,
            pltpu.SMEM((BINS + 8, 128), jnp.int32),
            pltpu.SemaphoreType.DMA,
            pltpu.VMEM((BINS, DEPTH, 128), BF16),
            pltpu.VMEM((BINS, 16, 128), BF16),
            pltpu.VMEM((BINS + 1, 16, 128), F32),
            *pipeline_scratch(),
        ],
        compiler_params=pltpu.CompilerParams(vmem_limit_bytes=16 << 20),
        cost_estimate=pl.CostEstimate(flops=10**9, bytes_accessed=10**6, transcendentals=0),
        name="own_tiles",
    )(own_table, packed)

    upward = (1 - lax.axis_index("slab") % 2).astype(jnp.int32)[None]
    new_velocity, new_force = pl.pallas_call(
        cross_kernel,
        out_shape=(cells, cells),
        in_specs=[SMEM] + [VMEM] * 8,
        out_specs=(VMEM, VMEM),
        scratch_shapes=[
            pltpu.VMEM((2 * BINS, DEPTH, 128), BF16),
            pltpu.VMEM((2 * BINS, 16, 128), BF16),
            pltpu.VMEM((2 * BINS, 1, 128), F32),
            pltpu.VMEM((BINS, 16, 128), F32),
            pltpu.VMEM((BINS + 8, 128), jnp.int32),
            pltpu.SMEM((BINS + 8, 128), jnp.int32),
            pltpu.SemaphoreType.DMA,
            *pipeline_scratch(),
        ],
        compiler_params=pltpu.CompilerParams(vmem_limit_bytes=16 << 20),
        cost_estimate=pl.CostEstimate(flops=10**9, bytes_accessed=10**6, transcendentals=0),
        name="cross_tiles",
    )(upward, odd, even, packed, velocity, old_force, acc, lt, ra)
    return tuple(map(by_component, (new_positions, new_velocity, new_force)))


def solution(mesh):
    flat = P(("slab", "blk"))
    rows = P(("slab", "blk"), None)
    cells = P(("slab", "blk"), None, None)
    return jax.shard_map(
        local,
        mesh=mesh,
        in_specs=(cells, rows, cells, cells, rows, flat),
        out_specs=(cells, cells, cells),
        check_vma=False,
    )
```
